256 devices in a mesh: grp: 8 (over z_lo, core), dev: 32 (over x, z_hi, y).
Axes of the slice: x: 4, y: 4, z: 8 (z_hi: 2, z_lo: 4; z = z_hi * 4 + z_lo), core: 2. Of those that a mesh axis runs over, the one named last changes fastest.
Arguments:
- centres: bfloat16 [524288, 512], P(('grp', 'dev')), may hold values from -12 to 12
- coefficients: float32 [100, 524288], P(None, ('grp', 'dev')), may hold values from -0.078125 to 0.078125
- targets: float32 [100, 4096], P(None, ('grp', 'dev')), may hold values from -6 to 6
- batch_index: int32 [4096], P(('grp', 'dev')), may hold values from 0 to 2047
- nys_index: int32 [4096], P(('grp', 'dev')), may hold values from 0 to 2047
- eigvecs: float32 [4096, 128], P(('grp', 'dev')), may hold values from -0.09375 to 0.09375
- eig_scale: float32 [128], replicated, may hold values from 0.1 to 2
Outputs:
- updated: float32 [100, 524288], P(None, ('grp', 'dev'))
- residual: float32 [100, 4096], P(None, ('grp', 'dev'))
The draws below stay inside these ranges and needn't reach their ends.
Inputs may be any that keep to these rules, and one draw needn't show every extreme that they name: `batch_index`: entries of the k-th block of 16 name rows within the k-th block of 2048 centres. `nys_index`: entries of the k-th block of 16 name rows within the k-th block of 2048 centres.
All inputs are finite; a program needn't handle non-finite values.
Results may differ from the reference program's by a relative error of at most 0.0031.
Values may be sent and summed in bfloat16 or wider, within the bound.
No kernel may reach another device: no remote copies, remote signals or barrier semaphores. Data moves between devices by JAX's collectives and lax.ppermute only.
A program may use at most 64 MiB of HBM per device.

```python
import math
import jax
import jax.numpy as jnp
from jax import lax

D = 512
O = 100
Q = 128
C_DEV = 2048
B_DEV = 16
S_DEV = 16
NC = 524288
BATCH = 4096
SUB = 4096
N_GRP = 8
N_DEV = 32


cluster_count = 16


def draw_centres(key, part):
    key_base = jax.random.fold_in(key, 11)
    key_scale = jax.random.fold_in(key, 12)
    key_means = jax.random.fold_in(key, 13)
    key_member = jax.random.fold_in(key, 14)
    member = jax.random.randint(key_member, (NC,), 0, cluster_count)
    means = 0.9 * jax.random.normal(key_means, (cluster_count, D), jnp.float32)
    noise = jnp.clip(jax.random.normal(key_base, (NC, D), jnp.float32), -4.0, 4.0)
    scales = jnp.exp(jax.random.uniform(key_scale, (NC, 1), jnp.float32, math.log(0.5), math.log(2.0)))
    rows = jnp.take(means, member, axis=0) + noise
    return jnp.clip(rows * scales, -12.0, 12.0).astype(jnp.bfloat16)


def set_ends(values, stream_key, smallest, largest):
    longest = values.shape.index(max(values.shape))
    spots = []
    for shift in (0, 1):
        where = [jax.random.randint(jax.random.fold_in(stream_key, axis), (), 0, length) for axis, length in enumerate(values.shape)]
        where[longest] = (where[longest] + shift) % values.shape[longest]
        spots.append(tuple(where))
    return values.at[spots[0]].set(smallest).at[spots[1]].set(largest)


def levels(rng, dims, cuts, smallest, largest):
    gain, own = 1.0, jax.random.fold_in(rng, 6)
    for position, parts in cuts:
        heights = jnp.exp(jax.random.uniform(jax.random.fold_in(own, position), (parts,), jnp.float32, smallest / len(cuts), largest / len(cuts)))
        gain = gain * jnp.repeat(heights, dims[position] // parts).reshape([-1 if axis == position else 1 for axis in range(len(dims))])
    return gain


def normal_values(key, shape, width, reach, cuts=(), kind=jnp.bfloat16):
    factor_of = levels(key, shape, cuts, -0.22, 0.18) if cuts else 1.0
    entries = jax.random.normal(key, shape, jnp.float32) * width * factor_of
    return jnp.minimum(jnp.maximum(entries, -reach), reach).astype(kind)


def setup_inputs(seed: int = 0) -> dict:
    key_list = jax.random.split(jax.random.key(seed), 8)
    centres = draw_centres(jax.random.fold_in(key_list[7], 71), 0)
    coefficients = normal_values(key_list[1], (O, NC), (NC // 100) ** -0.5, 0.078125, ((1, 256),), jnp.float32)
    targets = normal_values(key_list[2], (O, BATCH), 1.0, 6.0, ((1, 256),), jnp.float32)
    batch_index = set_ends(jax.random.randint(key_list[3], (BATCH,), 0, C_DEV), jax.random.fold_in(key_list[3], 1), 0, C_DEV - 1).astype(jnp.int32)
    nys_index = set_ends(jax.random.randint(key_list[4], (SUB,), 0, C_DEV), jax.random.fold_in(key_list[4], 1), 0, C_DEV - 1).astype(jnp.int32)
    eigvecs = normal_values(key_list[5], (SUB, Q), SUB ** -0.5, 0.09375, ((0, 256),), jnp.float32)
    eig_scale = jnp.clip(jnp.exp(jax.random.uniform(key_list[6], (Q,), jnp.float32, math.log(0.1), math.log(2.0))), 0.1, 2.0)
    return dict(centres=centres, coefficients=coefficients, targets=targets, batch_index=batch_index, nys_index=nys_index, eigvecs=eigvecs, eig_scale=eig_scale)


step_rate = 1.0

def kernel_block(left_rows, right_rows, spread):
    left_sq = lax.optimization_barrier(jnp.sum(jnp.square(left_rows.astype(jnp.float32)), axis=1))
    right_sq = lax.optimization_barrier(jnp.sum(jnp.square(right_rows.astype(jnp.float32)), axis=1))
    cross_dot = lax.dot_general(left_rows, right_rows, (((1,), (1,)), ((), ())), preferred_element_type=jnp.float32)
    distance = jnp.sqrt(jnp.maximum(left_sq[:, None] + right_sq[None, :] - 2.0 * cross_dot, 1.0))
    return jnp.exp(-distance / spread)

def reference(centres, coefficients, targets, batch_index, nys_index, eigvecs, eig_scale):
    spread = 0.7 * math.sqrt(D)
    shards = N_GRP * N_DEV
    batch_global = jnp.arange(BATCH, dtype=jnp.int32) // B_DEV * C_DEV + batch_index.astype(jnp.int32)
    nys_global = jnp.arange(SUB, dtype=jnp.int32) // S_DEV * C_DEV + nys_index.astype(jnp.int32)
    batch_rows = centres[batch_global]
    nys_rows = centres[nys_global]
    coef_bf = coefficients.astype(jnp.bfloat16)
    centre_blocks = centres.reshape(shards, C_DEV, D)
    coef_blocks = jnp.transpose(coef_bf.reshape(O, shards, C_DEV), (1, 0, 2))

    def add_shard(running, block_pair):
        centre_block, coef_block = block_pair
        kernel = kernel_block(batch_rows, centre_block, spread).astype(jnp.bfloat16)
        partial_value = lax.dot_general(coef_block, kernel, (((1,), (1,)), ((), ())), preferred_element_type=jnp.float32)
        return (running + partial_value, None)
    predicted, _ = lax.scan(add_shard, jnp.zeros((O, BATCH), jnp.float32), (centre_blocks, coef_blocks))
    residual = predicted - targets
    nys_kernel = kernel_block(nys_rows, batch_rows, spread)
    nys_sums = lax.dot_general(nys_kernel, residual, (((1,), (1,)), ((), ())), precision=lax.Precision.HIGHEST)
    projected = lax.dot_general(eigvecs, nys_sums, (((0,), (0,)), ((), ())), precision=lax.Precision.HIGHEST)
    correction = jnp.dot(eigvecs, eig_scale[:, None] * projected, precision=lax.Precision.HIGHEST)
    updated = coefficients.at[:, batch_global].add(-step_rate * residual)
    updated = updated.at[:, nys_global].add(step_rate * jnp.transpose(correction))
    return (updated, residual)
```

```python
import functools
import math

import jax
import jax.numpy as jnp
from jax import lax
from jax.experimental import pallas as pl
from jax.experimental.pallas import tpu as pltpu
from jax.sharding import PartitionSpec as P


step_rate = 1.0
LANES = 128
BOTH = ("grp", "dev")
F32 = jnp.float32
BF16 = jnp.bfloat16
HIGHEST = lax.Precision.HIGHEST

NX, NY, NZ = 4, 4, 8


def place(x, y, z, core):
    return ((z % 4) * 2 + core) * 32 + x * 8 + (z // 4) * 4 + y


def route(target):
    pairs = []
    for x in range(NX):
        for y in range(NY):
            for z in range(NZ):
                for core in range(2):
                    tx, ty, tz, tc = target(x, y, z, core)
                    pairs.append((place(x, y, z, core), place(tx % NX, ty % NY, tz % NZ, tc)))
    return pairs


def turned(core, first, second):
    return (first, second) if core == 0 else (second, first)


def plane_route(first, second):
    def target(x, y, z, core):
        dx, dy = turned(core, first, second)
        return x + dx, y + dy, z, core

    return route(target)


def z_route(k):
    return route(lambda x, y, z, core: (x, y, z + k, core))


CORE = route(lambda x, y, z, core: (x, y, z, 1 - core))


def move(x, pairs):
    return lax.ppermute(x, BOTH, pairs)


def laplace(cross, left_sq, right_sq, factor):
    v = jnp.maximum(cross + left_sq + right_sq, 1.0)
    return jnp.exp2((v * factor) * lax.rsqrt(v))


def nt_dot(a, b):
    return lax.dot_general(a, b, (((1,), (1,)), ((), ())), preferred_element_type=F32)


def score_kernel(factor, sub, rows_ref, own_ref, peer_ref, own_w_ref, peer_w_ref, own_sq_ref, peer_sq_ref,
                 nys_ref, nys_sq_ref, basis_ref, out_ref, scaled, row_sq, total):
    step = pl.program_id(0)
    count = rows_ref.shape[0]

    @pl.when(step == 0)
    def _():
        for r in range(0, count, sub):
            wide = rows_ref[r : r + sub, :].astype(F32)
            row_sq[r : r + sub, :] = jnp.broadcast_to(
                jnp.sum(wide * wide, axis=1, keepdims=True), (sub, LANES)
            )
            scaled[r : r + sub, :] = (wide * -2.0).astype(BF16)
        total[...] = jnp.zeros_like(total)

    for centre_ref, w_ref, sq_ref in ((own_ref, own_w_ref, own_sq_ref), (peer_ref, peer_w_ref, peer_sq_ref)):
        for r in range(0, count, sub):
            cross = nt_dot(scaled[r : r + sub, :], centre_ref[...])
            kernel = laplace(cross, row_sq[r : r + sub, 0:1], sq_ref[...], factor).astype(BF16)
            total[r : r + sub, :] += jnp.dot(kernel, w_ref[...], preferred_element_type=F32)

    @pl.when(step == pl.num_programs(0) - 1)
    def _():
        for r in range(0, count, sub):
            cross = nt_dot(scaled[r : r + sub, :], nys_ref[...])
            kernel = laplace(cross, row_sq[r : r + sub, 0:1], nys_sq_ref[...], factor)
            basis = jnp.dot(kernel, basis_ref[...], precision=HIGHEST, preferred_element_type=F32)
            out_ref[r : r + sub, 0:LANES] = total[r : r + sub, :].astype(BF16)
            out_ref[r : r + sub, LANES : 2 * LANES] = basis.astype(BF16)


def score(rows, own, peer, own_w, peer_w, own_sq, peer_sq, nys, nys_sq, basis, factor):
    count, dim = rows.shape
    tile = 256
    steps = own.shape[0] // tile
    whole = lambda a: pl.BlockSpec(a.shape, lambda i: (0, 0))
    down = lambda a: pl.BlockSpec((tile, a.shape[1]), lambda i: (i, 0))
    along = pl.BlockSpec((1, tile), lambda i: (0, i))
    pairs = count * 2 * own.shape[0]
    return pl.pallas_call(
        functools.partial(score_kernel, factor, 256),
        grid=(steps,),
        in_specs=[whole(rows), down(own), down(peer), down(own_w), down(peer_w), along, along,
                  whole(nys), whole(nys_sq), whole(basis)],
        out_specs=pl.BlockSpec((count, 2 * LANES), lambda i: (0, 0)),
        out_shape=jax.ShapeDtypeStruct((count, 2 * LANES), BF16),
        scratch_shapes=[pltpu.VMEM((count, dim), BF16), pltpu.VMEM((count, LANES), F32), pltpu.VMEM((count, LANES), F32)],
        cost_estimate=pl.CostEstimate(flops=2 * pairs * (dim + LANES), bytes_accessed=pairs, transcendentals=2 * pairs),
        compiler_params=pltpu.CompilerParams(vmem_limit_bytes=16 * 1024 * 1024),
    )(rows, own, peer, own_w, peer_w, own_sq, peer_sq, nys, nys_sq, basis)


def pick_kernel(index_ref, column_ref, centres_ref, out_ref, held, sems):
    count = out_ref.shape[0]
    copies = []
    for r in range(count):
        start = pl.multiple_of((index_ref[r] // 8) * 8, 8)
        copy = pltpu.make_async_copy(centres_ref.at[pl.ds(start, 8), :], held.at[pl.ds(8 * r, 8), :], sems.at[r])
        copy.start()
        copies.append(copy)
    for copy in copies:
        copy.wait()
    row = lax.broadcasted_iota(jnp.int32, (count, 8 * count), 0)
    column = lax.broadcasted_iota(jnp.int32, (count, 8 * count), 1)
    chosen = (column == 8 * row + (column_ref[...] & 7)).astype(F32).astype(BF16)
    out_ref[...] = jnp.dot(chosen, held[...], preferred_element_type=F32).astype(BF16)


def pick_rows(index, centres):
    count, dim = index.shape[0], centres.shape[1]
    return pl.pallas_call(
        pick_kernel,
        in_specs=[
            pl.BlockSpec(memory_space=pltpu.SMEM),
            pl.BlockSpec(memory_space=pltpu.VMEM),
            pl.BlockSpec(memory_space=pl.ANY),
        ],
        out_specs=pl.BlockSpec(memory_space=pltpu.VMEM),
        out_shape=jax.ShapeDtypeStruct((count, dim), BF16),
        scratch_shapes=[pltpu.VMEM((8 * count, dim), BF16), pltpu.SemaphoreType.DMA((count,))],
        compiler_params=pltpu.CompilerParams(vmem_limit_bytes=8 * 1024 * 1024),
    )(index, index[:, None], centres)


def squares(rows):
    return jnp.sum(jnp.square(rows.astype(F32)), axis=1)[None, :]


def per_device(centres, coefficients, targets, batch_index, nys_index, eigvecs, eig_scale):
    own_centres, dim = centres.shape
    outputs = coefficients.shape[0]
    own_batch = targets.shape[1]
    own_nys = nys_index.shape[0]
    factor = -math.log2(math.e) / (0.7 * math.sqrt(dim))
    core = lax.axis_index("grp") % 2

    picked = pick_rows(jnp.concatenate([batch_index, nys_index]), centres)
    own_rows, nys_rows = picked[:own_batch], picked[own_batch:]

    weights = jnp.pad(coefficients.astype(BF16), ((0, LANES - outputs), (0, 0))).T
    centre_sq = squares(centres)
    peer_centres = move(centres, CORE)
    peer_weights = move(weights, CORE)
    peer_sq = move(centre_sq, CORE)

    pieces = [own_rows] + [move(own_rows, z_route(-k)) for k in range(1, NZ)]
    line = jnp.concatenate(pieces, axis=0)
    peer_nys = move(nys_rows, CORE)
    peer_eig = move(eigvecs, CORE)
    nys_all = jnp.concatenate([nys_rows, peer_nys], axis=0)
    nys_sq = squares(nys_all)
    basis = jnp.concatenate([eigvecs, peer_eig], axis=0)
    shifts = (0, 1, 3, 2)
    sheet = jnp.concatenate([line if a == 0 else move(line, plane_route(-a, 0)) for a in shifts], axis=0)
    groups = [sheet if b == 0 else move(sheet, plane_route(0, -b)) for b in shifts]

    block = line.shape[0]
    returned = []
    for b, rows in zip(shifts, groups):
        part = score(rows, centres, peer_centres, weights, peer_weights, centre_sq, peer_sq,
                     nys_all, nys_sq, basis, factor)
        for i, a in enumerate(shifts):
            mine = part[i * block : (i + 1) * block]
            returned.append(mine if (a, b) == (0, 0) else move(mine, plane_route(a, b)))
    line_sum = functools.reduce(lambda s, r: s + r.astype(F32), returned[1:], returned[0].astype(F32))

    mine = line_sum[:own_batch]
    for k in range(1, NZ):
        mine = mine + move(line_sum[k * own_batch : (k + 1) * own_batch], z_route(k))
    residual_rows = mine[:, :outputs] - targets.T
    basis_rows = mine[:, LANES:]
    residual_own = residual_rows.T

    part = lax.dot_general(basis_rows, residual_rows, (((0,), (0,)), ((), ())), precision=HIGHEST)
    half = part.shape[0] // 2
    part = jnp.pad(part, ((0, 0), (0, LANES - outputs)))
    part = part + move(part, CORE)
    part = lax.dynamic_slice_in_dim(part, core * half, half, 0)
    part = functools.reduce(jnp.add, [move(part, z_route(k)) for k in range(1, NZ)], part)
    part = functools.reduce(jnp.add, [move(part, plane_route(k, 0)) for k in (1, 3, 2)], part)
    part = functools.reduce(jnp.add, [move(part, plane_route(0, k)) for k in (1, 3, 2)], part)
    other = move(part, CORE)
    projected = jnp.where(
        core == 0, jnp.concatenate([part, other], axis=0), jnp.concatenate([other, part], axis=0)
    )[:, :outputs]
    correction = jnp.dot(eigvecs, eig_scale[:, None] * projected, precision=HIGHEST)

    columns = lax.broadcasted_iota(jnp.int32, (own_batch + own_nys, own_centres), 1)
    chosen = (jnp.concatenate([batch_index, nys_index])[:, None] == columns).astype(F32)
    change = jnp.concatenate([-step_rate * residual_rows, step_rate * correction], axis=0)
    updated = coefficients + lax.dot_general(change, chosen, (((0,), (0,)), ((), ())), precision=HIGHEST)
    return (updated, residual_own)


def solution(mesh):
    in_specs = (
        P(BOTH, None),
        P(None, BOTH),
        P(None, BOTH),
        P(BOTH),
        P(BOTH),
        P(BOTH, None),
        P(),
    )
    out_specs = (P(None, BOTH), P(None, BOTH))
    return jax.shard_map(per_device, mesh=mesh, in_specs=in_specs, out_specs=out_specs, check_vma=False)
```

```python
import functools
import math

import jax
import jax.numpy as jnp
from jax import lax
from jax.experimental import pallas as pl
from jax.experimental.pallas import tpu as pltpu
from jax.sharding import PartitionSpec as P


step_rate = 1.0
LANES = 128
BOTH = ("grp", "dev")
F32 = jnp.float32
BF16 = jnp.bfloat16
HIGHEST = lax.Precision.HIGHEST

NX, NY, NZ = 4, 4, 8


def place(x, y, z, core):
    return ((z % 4) * 2 + core) * 32 + x * 8 + (z // 4) * 4 + y


def route(target):
    pairs = []
    for x in range(NX):
        for y in range(NY):
            for z in range(NZ):
                for core in range(2):
                    tx, ty, tz, tc = target(x, y, z, core)
                    pairs.append((place(x, y, z, core), place(tx % NX, ty % NY, tz % NZ, tc)))
    return pairs


def turned(core, first, second):
    return (first, second) if core == 0 else (second, first)


def plane_route(first, second):
    def target(x, y, z, core):
        dx, dy = turned(core, first, second)
        return x + dx, y + dy, z, core

    return route(target)


def z_route(k):
    return route(lambda x, y, z, core: (x, y, z + k, core))


CORE = route(lambda x, y, z, core: (x, y, z, 1 - core))


def move(x, pairs):
    return lax.ppermute(x, BOTH, pairs)


def laplace(cross, left_sq, right_sq, factor):
    v = jnp.maximum(cross + left_sq + right_sq, 1.0)
    return jnp.exp2((v * factor) * lax.rsqrt(v))


def nt_dot(a, b):
    return lax.dot_general(a, b, (((1,), (1,)), ((), ())), preferred_element_type=F32)


def whole(space=pltpu.VMEM):
    return pl.BlockSpec(memory_space=space)


def score_kernel(factor, tile, rows_ref, own_ref, peer_ref, own_w_ref, peer_w_ref, own_sq_ref, peer_sq_ref,
                 nys_ref, nys_sq_ref, basis_ref, out_ref, scaled, row_sq, total):
    count = rows_ref.shape[0]
    wide = rows_ref[...].astype(F32)
    row_sq[...] = jnp.broadcast_to(jnp.sum(wide * wide, axis=1, keepdims=True), (count, LANES))
    scaled[...] = (wide * -2.0).astype(BF16)
    total[...] = jnp.zeros_like(total)

    def one_tile(t, carry):
        at = pl.ds(pl.multiple_of(t * tile, tile), tile)
        sides = ((own_ref, own_w_ref, own_sq_ref), (peer_ref, peer_w_ref, peer_sq_ref))
        crosses = [nt_dot(scaled[...], centre_ref[at, :]) for centre_ref, _, _ in sides]
        for cross, (_, w_ref, sq_ref) in zip(crosses, sides):
            kernel = laplace(cross, row_sq[:, 0:1], sq_ref[:, at], factor).astype(BF16)
            total[...] += nt_dot(kernel, w_ref[:, at])
        return carry

    lax.fori_loop(0, own_ref.shape[0] // tile, one_tile, 0)
    cross = nt_dot(scaled[...], nys_ref[...])
    kernel = laplace(cross, row_sq[:, 0:1], nys_sq_ref[...], factor)
    basis = jnp.dot(kernel, basis_ref[...], precision=HIGHEST, preferred_element_type=F32)
    out_ref[:, 0:LANES] = total[...].astype(BF16)
    out_ref[:, LANES : 2 * LANES] = basis.astype(BF16)


def score(rows, own, peer, own_w, peer_w, own_sq, peer_sq, nys, nys_sq, basis, factor):
    count, dim = rows.shape
    pairs = count * 2 * own.shape[0]
    return pl.pallas_call(
        functools.partial(score_kernel, factor, 256),
        in_specs=[whole()] * 10,
        out_specs=whole(),
        out_shape=jax.ShapeDtypeStruct((count, 2 * LANES), BF16),
        scratch_shapes=[pltpu.VMEM((count, dim), BF16), pltpu.VMEM((count, LANES), F32), pltpu.VMEM((count, LANES), F32)],
        cost_estimate=pl.CostEstimate(flops=2 * pairs * (dim + LANES), bytes_accessed=pairs, transcendentals=2 * pairs),
        compiler_params=pltpu.CompilerParams(vmem_limit_bytes=24 * 1024 * 1024),
    )(rows, own, peer, own_w, peer_w, own_sq, peer_sq, nys, nys_sq, basis)


def pick_kernel(batch_ref, nys_ref, centres_ref, batch_out, nys_out, held, sems):
    copies = []
    count = batch_out.shape[0]
    row = lax.broadcasted_iota(jnp.int32, (2 * count, 16 * count), 0)
    column = lax.broadcasted_iota(jnp.int32, (2 * count, 16 * count), 1)
    target = jnp.zeros_like(column)
    for r in range(2 * count):
        index = batch_ref[r] if r < count else nys_ref[r - count]
        start = pl.multiple_of((index // 8) * 8, 8)
        copy = pltpu.make_async_copy(centres_ref.at[pl.ds(start, 8), :], held.at[pl.ds(8 * r, 8), :], sems.at[r])
        copy.start()
        copies.append(copy)
        target = jnp.where(row == r, 8 * r + (index & 7), target)
    for copy in copies:
        copy.wait()
    chosen = (column == target).astype(F32).astype(BF16)
    rows = jnp.dot(chosen, held[...], preferred_element_type=F32).astype(BF16)
    batch_out[...] = rows[:count]
    nys_out[...] = rows[count:]


def pick_rows(batch_index, nys_index, centres):
    count, dim = batch_index.shape[0], centres.shape[1]
    return pl.pallas_call(
        pick_kernel,
        in_specs=[whole(pltpu.SMEM), whole(pltpu.SMEM), whole(pltpu.HBM)],
        out_specs=[whole(), whole()],
        out_shape=[jax.ShapeDtypeStruct((count, dim), BF16)] * 2,
        scratch_shapes=[pltpu.VMEM((16 * count, dim), BF16), pltpu.SemaphoreType.DMA((2 * count,))],
        compiler_params=pltpu.CompilerParams(vmem_limit_bytes=8 * 1024 * 1024),
    )(batch_index, nys_index, centres)


def line_kernel(z_ref, parts_ref, targets_ref, out_ref):
    outputs, own = targets_ref.shape
    copies, count = out_ref.shape[0], out_ref.shape[1]
    total = parts_ref[0]
    for i in range(1, parts_ref.shape[0]):
        total = total + parts_ref[i]
    padded = jnp.concatenate([targets_ref[...], jnp.zeros((LANES - outputs, own), F32)], axis=0)
    padded = jnp.concatenate([padded] * (LANES // own), axis=1).T
    row = lax.broadcasted_iota(jnp.int32, (count, LANES), 0)
    mine = (row >= z_ref[0] * own) & (row < z_ref[0] * own + own)
    left = (total[:, :LANES] - jnp.where(mine, padded, 0.0)).astype(BF16)
    right = total[:, LANES:].astype(BF16)
    for i in range(copies):
        out_ref[i, :, 0:LANES] = left
        out_ref[i, :, LANES : 2 * LANES] = right


def line_sum(z, parts, targets, copies):
    return pl.pallas_call(
        line_kernel,
        in_specs=[whole(pltpu.SMEM), whole(), whole()],
        out_specs=whole(),
        out_shape=jax.ShapeDtypeStruct((copies, parts.shape[1], parts.shape[2]), BF16),
        compiler_params=pltpu.CompilerParams(vmem_limit_bytes=8 * 1024 * 1024),
    )(z, parts, targets)


def product_kernel(z_ref, parts_ref, part_ref, rows_ref, held):
    own = rows_ref.shape[0]
    total = parts_ref[0].astype(F32)
    for i in range(1, parts_ref.shape[0]):
        total = total + parts_ref[i].astype(F32)
    residual = total[:, :LANES]
    held[...] = residual
    part_ref[...] = lax.dot_general(
        total[:, LANES:], residual, (((0,), (0,)), ((), ())), precision=HIGHEST, preferred_element_type=F32
    )
    rows_ref[...] = held[pl.ds(pl.multiple_of(z_ref[0] * own, own), own), :]


def product(z, parts, own):
    return pl.pallas_call(
        product_kernel,
        in_specs=[whole(pltpu.SMEM), whole()],
        out_specs=[whole(), whole()],
        out_shape=[jax.ShapeDtypeStruct((LANES, LANES), F32), jax.ShapeDtypeStruct((own, LANES), F32)],
        scratch_shapes=[pltpu.VMEM((parts.shape[1], LANES), F32)],
        compiler_params=pltpu.CompilerParams(vmem_limit_bytes=8 * 1024 * 1024),
    )(z, parts)


Z_GROUPS = [[place(x, y, z, core) for z in range(NZ)] for x in range(NX) for y in range(NY) for core in range(2)]
FIRST_GROUPS = [[place(i, y, z, 0) for i in range(NX)] for y in range(NY) for z in range(NZ)] + [
    [place(x, i, z, 1) for i in range(NY)] for x in range(NX) for z in range(NZ)
]


def exchange(blocks, groups):
    return lax.all_to_all(blocks, BOTH, split_axis=0, concat_axis=0, tiled=True, axis_index_groups=groups)


def gather(x, groups):
    count = len(groups[0])
    blocks = exchange(jnp.broadcast_to(x, (count, *x.shape)), groups)
    return blocks.reshape(count * x.shape[0], x.shape[1])


def squares(rows):
    return jnp.sum(jnp.square(rows.astype(F32)), axis=1)[None, :]


def per_device(centres, coefficients, targets, batch_index, nys_index, eigvecs, eig_scale):
    own_centres, dim = centres.shape
    outputs = coefficients.shape[0]
    own_batch = targets.shape[1]
    own_nys = nys_index.shape[0]
    factor = -math.log2(math.e) / (0.7 * math.sqrt(dim))
    z = ((lax.axis_index("dev") // 4) % 2 * 4 + lax.axis_index("grp") // 2)[None]

    peer_centres = move(centres, CORE)
    own_rows, nys_rows = pick_rows(batch_index, nys_index, centres)
    weights = jnp.pad(coefficients.astype(BF16), ((0, LANES - outputs), (0, 0)))
    peer_weights = move(weights, CORE)
    peer_nys = move(nys_rows, CORE)
    peer_eig = move(eigvecs, CORE)

    line = gather(own_rows, Z_GROUPS)
    sheet = gather(line, FIRST_GROUPS)
    shifts = (0, 1, 3, 2)
    groups = [sheet if b == 0 else move(sheet, plane_route(0, -b)) for b in shifts]
    nys_all = jnp.concatenate([nys_rows, peer_nys], axis=0)
    nys_sq = squares(nys_all)
    basis = jnp.concatenate([eigvecs, peer_eig], axis=0)
    centre_sq = squares(centres)
    peer_sq = squares(peer_centres)

    returned = []
    for b, rows in zip(shifts, groups):
        part = score(rows, centres, peer_centres, weights, peer_weights, centre_sq, peer_sq,
                     nys_all, nys_sq, basis, factor)
        returned.append(part if b == 0 else move(part, plane_route(0, b)))
    sheet_sum = functools.reduce(lambda s, r: s + r.astype(F32), returned[1:], returned[0].astype(F32))

    parts = exchange(sheet_sum.reshape(NX, line.shape[0], 2 * LANES), FIRST_GROUPS)
    lines = exchange(line_sum(z, parts, targets, NZ), Z_GROUPS)
    part, residual_rows = product(z, lines, own_batch)
    residual_rows = residual_rows[:, :outputs]
    residual_own = residual_rows.T

    part = (part + move(part, CORE)).astype(BF16)
    others = [move(part, plane_route(a, b)) for a in range(NX) for b in range(NY) if a or b]
    projected = functools.reduce(lambda s, r: s + r.astype(F32), others, part.astype(F32))[:, :outputs]
    correction = jnp.dot(eigvecs, eig_scale[:, None] * projected, precision=HIGHEST)

    columns = lax.broadcasted_iota(jnp.int32, (own_batch + own_nys, own_centres), 1)
    chosen = (jnp.concatenate([batch_index, nys_index])[:, None] == columns).astype(F32)
    change = jnp.concatenate([-step_rate * residual_rows, step_rate * correction], axis=0)
    updated = coefficients + lax.dot_general(change, chosen, (((0,), (0,)), ((), ())), precision=HIGHEST)
    return (updated, residual_own)


def solution(mesh):
    in_specs = (
        P(BOTH, None),
        P(None, BOTH),
        P(None, BOTH),
        P(BOTH),
        P(BOTH),
        P(BOTH, None),
        P(),
    )
    out_specs = (P(None, BOTH), P(None, BOTH))
    return jax.shard_map(per_device, mesh=mesh, in_specs=in_specs, out_specs=out_specs, check_vma=False)
```

```python
import functools
import math

import jax
import jax.numpy as jnp
from jax import lax
from jax.experimental import pallas as pl
from jax.experimental.pallas import tpu as pltpu
from jax.sharding import PartitionSpec as P


step_rate = 1.0
LANES = 128
TILE = 512
BOTH = ("grp", "dev")
F32 = jnp.float32
BF16 = jnp.bfloat16
HIGHEST = lax.Precision.HIGHEST

NX, NY, NZ = 4, 4, 8


def place(x, y, z, core):
    return ((z % 4) * 2 + core) * 32 + x * 8 + (z // 4) * 4 + y


def route(target):
    pairs = []
    for x in range(NX):
        for y in range(NY):
            for z in range(NZ):
                for core in range(2):
                    tx, ty, tz, tc = target(x, y, z, core)
                    pairs.append((place(x, y, z, core), place(tx % NX, ty % NY, tz % NZ, tc)))
    return pairs


def turned(core, first, second):
    return (first, second) if core == 0 else (second, first)


def plane_route(first, second):
    def target(x, y, z, core):
        dx, dy = turned(core, first, second)
        return x + dx, y + dy, z, core

    return route(target)


def z_route(k):
    return route(lambda x, y, z, core: (x, y, z + k, core))


CORE = route(lambda x, y, z, core: (x, y, z, 1 - core))


def move(x, pairs):
    return lax.ppermute(x, BOTH, pairs)


def laplace(cross, left_sq, right_sq, factor):
    v = jnp.maximum(cross + left_sq + right_sq, 1.0)
    return jnp.exp2((v * factor) * lax.rsqrt(v))


def whole(space=pltpu.VMEM):
    return pl.BlockSpec(memory_space=space)


def nn_dot(a, b):
    return jnp.dot(a, b, preferred_element_type=F32)


def upright(row):
    return jnp.broadcast_to(row, (LANES, row.shape[1])).T[:, 0:1]


def score_kernel(factor, fetch, rows_ref, own_ref, peer_ref, own_w_ref, peer_w_ref, own_sq_ref, peer_sq_ref,
                 nys_ref, nys_sq_ref, basis_ref, out_ref, *rest):
    turned = rest[2] if fetch else rest[0]
    fetches = []
    if fetch:
        sems = rest[3]
        for i, (source, held) in enumerate(((peer_ref, rest[0]), (peer_w_ref, rest[1]))):
            fetches.append(pltpu.make_async_copy(source, held, sems.at[i]))
            fetches[i].start()
        peer_ref, peer_w_ref = rest[0], rest[1]
    count = rows_ref.shape[0]
    flat = rows_ref[...].astype(F32).T
    row_sq = jnp.sum(flat * flat, axis=0, keepdims=True)
    turned[...] = (flat * -2.0).astype(BF16)
    sides = ((own_ref, own_w_ref, own_sq_ref), (peer_ref, peer_w_ref, peer_sq_ref))
    jobs = [(*side, slice(at, at + TILE)) for side in sides for at in range(0, own_ref.shape[0], TILE)]
    cross = nn_dot(own_ref[0:TILE, :], turned[...])
    total = jnp.zeros((LANES, count), F32)
    for i, (_, w_ref, sq_ref, at) in enumerate(jobs):
        ahead = None
        if i + 1 < len(jobs):
            if 2 * (i + 1) == len(jobs):
                for copy in fetches:
                    copy.wait()
            centre_ref, _, _, next_at = jobs[i + 1]
            ahead = nn_dot(centre_ref[next_at, :], turned[...])
        kernel = laplace(cross, upright(sq_ref[:, at]), row_sq, factor).astype(BF16)
        total = total + nn_dot(w_ref[:, at], kernel)
        cross = ahead
    kernel = laplace(nn_dot(nys_ref[...], turned[...]), upright(nys_sq_ref[...]), row_sq, factor)
    basis = lax.dot_general(
        basis_ref[...], kernel, (((0,), (0,)), ((), ())), precision=HIGHEST, preferred_element_type=F32
    )
    out_ref[:, 0:LANES] = total.T.astype(BF16)
    out_ref[:, LANES : 2 * LANES] = basis.T.astype(BF16)


def score(rows, own, peer, own_w, peer_w, own_sq, peer_sq, nys, nys_sq, basis, factor, fetch):
    count, dim = rows.shape
    pairs = count * 2 * own.shape[0]
    in_specs = [whole()] * 10
    out_shape = [jax.ShapeDtypeStruct((count, 2 * LANES), BF16)]
    scratch = [pltpu.VMEM((dim, count), BF16)]
    if fetch:
        in_specs[2] = in_specs[4] = whole(pl.ANY)
        out_shape += [jax.ShapeDtypeStruct(peer.shape, BF16), jax.ShapeDtypeStruct(peer_w.shape, BF16)]
        scratch.append(pltpu.SemaphoreType.DMA((2,)))
    return pl.pallas_call(
        functools.partial(score_kernel, factor, fetch),
        in_specs=in_specs,
        out_specs=[whole()] * len(out_shape),
        out_shape=out_shape,
        scratch_shapes=scratch,
        cost_estimate=pl.CostEstimate(flops=2 * pairs * (dim + LANES), bytes_accessed=pairs, transcendentals=2 * pairs),
        compiler_params=pltpu.CompilerParams(vmem_limit_bytes=16 * 1024 * 1024),
    )(rows, own, peer, own_w, peer_w, own_sq, peer_sq, nys, nys_sq, basis)


def pick_kernel(batch_ref, nys_ref, centres_ref, batch_out, nys_out, held, sems):
    copies = []
    count = batch_out.shape[0]
    row = lax.broadcasted_iota(jnp.int32, (2 * count, 16 * count), 0)
    column = lax.broadcasted_iota(jnp.int32, (2 * count, 16 * count), 1)
    target = jnp.zeros_like(column)
    for r in range(2 * count):
        index = batch_ref[r] if r < count else nys_ref[r - count]
        start = pl.multiple_of((index // 8) * 8, 8)
        copy = pltpu.make_async_copy(centres_ref.at[pl.ds(start, 8), :], held.at[pl.ds(8 * r, 8), :], sems.at[r])
        copy.start()
        copies.append(copy)
        target = jnp.where(row == r, 8 * r + (index & 7), target)
    for copy in copies:
        copy.wait()
    chosen = (column == target).astype(F32).astype(BF16)
    rows = jnp.dot(chosen, held[...], preferred_element_type=F32).astype(BF16)
    batch_out[...] = rows[:count]
    nys_out[...] = rows[count:]


def pick_rows(batch_index, nys_index, centres):
    count, dim = batch_index.shape[0], centres.shape[1]
    return pl.pallas_call(
        pick_kernel,
        in_specs=[whole(pltpu.SMEM), whole(pltpu.SMEM), whole(pltpu.HBM)],
        out_specs=[whole(), whole()],
        out_shape=[jax.ShapeDtypeStruct((count, dim), BF16)] * 2,
        scratch_shapes=[pltpu.VMEM((16 * count, dim), BF16), pltpu.SemaphoreType.DMA((2 * count,))],
        compiler_params=pltpu.CompilerParams(vmem_limit_bytes=8 * 1024 * 1024),
    )(batch_index, nys_index, centres)


def line_kernel(z_ref, parts_ref, targets_ref, out_ref):
    outputs, own = targets_ref.shape
    copies, count = out_ref.shape[0], out_ref.shape[1]
    total = parts_ref[0]
    for i in range(1, parts_ref.shape[0]):
        total = total + parts_ref[i]
    padded = jnp.concatenate([targets_ref[...], jnp.zeros((LANES - outputs, own), F32)], axis=0)
    padded = jnp.concatenate([padded] * (LANES // own), axis=1).T
    row = lax.broadcasted_iota(jnp.int32, (count, LANES), 0)
    mine = (row >= z_ref[0] * own) & (row < z_ref[0] * own + own)
    left = (total[:, :LANES] - jnp.where(mine, padded, 0.0)).astype(BF16)
    right = total[:, LANES:].astype(BF16)
    for i in range(copies):
        out_ref[i, :, 0:LANES] = left
        out_ref[i, :, LANES : 2 * LANES] = right


def line_sum(z, parts, targets, copies):
    return pl.pallas_call(
        line_kernel,
        in_specs=[whole(pltpu.SMEM), whole(), whole()],
        out_specs=whole(),
        out_shape=jax.ShapeDtypeStruct((copies, parts.shape[1], parts.shape[2]), BF16),
        compiler_params=pltpu.CompilerParams(vmem_limit_bytes=8 * 1024 * 1024),
    )(z, parts, targets)


def product_kernel(z_ref, parts_ref, part_ref, rows_ref, held):
    own = rows_ref.shape[0]
    total = parts_ref[0].astype(F32)
    for i in range(1, parts_ref.shape[0]):
        total = total + parts_ref[i].astype(F32)
    residual = total[:, :LANES]
    held[...] = residual
    part_ref[...] = lax.dot_general(
        total[:, LANES:], residual, (((0,), (0,)), ((), ())), precision=HIGHEST, preferred_element_type=F32
    )
    rows_ref[...] = held[pl.ds(pl.multiple_of(z_ref[0] * own, own), own), :]


def product(z, parts, own):
    return pl.pallas_call(
        product_kernel,
        in_specs=[whole(pltpu.SMEM), whole()],
        out_specs=[whole(), whole()],
        out_shape=[jax.ShapeDtypeStruct((LANES, LANES), F32), jax.ShapeDtypeStruct((own, LANES), F32)],
        scratch_shapes=[pltpu.VMEM((parts.shape[1], LANES), F32)],
        compiler_params=pltpu.CompilerParams(vmem_limit_bytes=8 * 1024 * 1024),
    )(z, parts)


Z_GROUPS = [[place(x, y, z, core) for z in range(NZ)] for x in range(NX) for y in range(NY) for core in range(2)]
PLANE_GROUPS = [[place(x, y, z, core) for x in range(NX) for y in range(NY)] for z in range(NZ) for core in range(2)]
FIRST_GROUPS = [[place(i, y, z, 0) for i in range(NX)] for y in range(NY) for z in range(NZ)] + [
    [place(x, i, z, 1) for i in range(NY)] for x in range(NX) for z in range(NZ)
]


def exchange(blocks, groups):
    return lax.all_to_all(blocks, BOTH, split_axis=0, concat_axis=0, tiled=True, axis_index_groups=groups)


def gather(x, groups):
    count = len(groups[0])
    blocks = exchange(jnp.broadcast_to(x, (count, *x.shape)), groups)
    return blocks.reshape(count * x.shape[0], x.shape[1])


def squares(rows):
    return jnp.sum(jnp.square(rows.astype(F32)), axis=1)[None, :]


def per_device(centres, coefficients, targets, batch_index, nys_index, eigvecs, eig_scale):
    own_centres, dim = centres.shape
    outputs = coefficients.shape[0]
    own_batch = targets.shape[1]
    own_nys = nys_index.shape[0]
    factor = -math.log2(math.e) / (0.7 * math.sqrt(dim))
    dev, grp = lax.axis_index("dev"), lax.axis_index("grp")
    z = (((dev >> 2) & 1) * 4 + (grp >> 1))[None]

    peer_centres = move(centres, CORE)
    own_rows, nys_rows = pick_rows(batch_index, nys_index, centres)
    weights = jnp.pad(coefficients.astype(BF16), ((0, LANES - outputs), (0, 0)))
    peer_weights = move(weights, CORE)
    peer_nys = move(nys_rows, CORE)
    peer_eig = move(eigvecs, CORE)

    line = gather(own_rows, Z_GROUPS)
    sheet = gather(line, FIRST_GROUPS)
    shifts = (0, 1, 3, 2)
    groups = [sheet if b == 0 else move(sheet, plane_route(0, -b)) for b in shifts]
    nys_all = jnp.concatenate([nys_rows, peer_nys], axis=0)
    nys_sq = squares(nys_all)
    basis = jnp.concatenate([eigvecs, peer_eig], axis=0)
    centre_sq = squares(centres)
    peer_sq = squares(peer_centres)

    returned = []
    for b, rows in zip(shifts, groups):
        part, *held = score(rows, centres, peer_centres, weights, peer_weights, centre_sq, peer_sq,
                            nys_all, nys_sq, basis, factor, b == 0)
        if held:
            peer_centres, peer_weights = held
        returned.append(part if b == 0 else move(part, plane_route(0, b)))
    sheet_sum = functools.reduce(lambda s, r: s + r.astype(F32), returned[1:], returned[0].astype(F32))

    parts = exchange(sheet_sum.reshape(NX, line.shape[0], 2 * LANES), FIRST_GROUPS)
    lines = exchange(line_sum(z, parts, targets, NZ), Z_GROUPS)
    part, residual_rows = product(z, lines, own_batch)
    residual_rows = residual_rows[:, :outputs]
    residual_own = residual_rows.T

    part = (part + move(part, CORE)).astype(BF16)
    parts = gather(part, PLANE_GROUPS).reshape(NX * NY, LANES, LANES)
    projected = jnp.sum(parts.astype(F32), axis=0)[:, :outputs]
    correction = jnp.dot(eigvecs, eig_scale[:, None] * projected, precision=HIGHEST)

    columns = lax.broadcasted_iota(jnp.int32, (own_batch + own_nys, own_centres), 1)
    chosen = (jnp.concatenate([batch_index, nys_index])[:, None] == columns).astype(F32)
    change = jnp.concatenate([-step_rate * residual_rows, step_rate * correction], axis=0)
    updated = coefficients + lax.dot_general(change, chosen, (((0,), (0,)), ((), ())), precision=HIGHEST)
    return (updated, residual_own)


def solution(mesh):
    in_specs = (
        P(BOTH, None),
        P(None, BOTH),
        P(None, BOTH),
        P(BOTH),
        P(BOTH),
        P(BOTH, None),
        P(),
    )
    out_specs = (P(None, BOTH), P(None, BOTH))
    return jax.shard_map(per_device, mesh=mesh, in_specs=in_specs, out_specs=out_specs, check_vma=False)
```

```python
import functools
import math

import jax
import jax.numpy as jnp
from jax import lax
from jax.experimental import pallas as pl
from jax.experimental.pallas import tpu as pltpu
from jax.sharding import PartitionSpec as P


step_rate = 1.0
LANES = 128
TILE = 512
BOTH = ("grp", "dev")
F32 = jnp.float32
BF16 = jnp.bfloat16
HIGHEST = lax.Precision.HIGHEST

NX, NY, NZ = 4, 4, 8


def place(x, y, z, core):
    return ((z % 4) * 2 + core) * 32 + x * 8 + (z // 4) * 4 + y


def route(target):
    pairs = []
    for x in range(NX):
        for y in range(NY):
            for z in range(NZ):
                for core in range(2):
                    tx, ty, tz, tc = target(x, y, z, core)
                    pairs.append((place(x, y, z, core), place(tx % NX, ty % NY, tz % NZ, tc)))
    return pairs


def turned(core, first, second):
    return (first, second) if core == 0 else (second, first)


def plane_route(first, second):
    def target(x, y, z, core):
        dx, dy = turned(core, first, second)
        return x + dx, y + dy, z, core

    return route(target)


def z_route(k):
    return route(lambda x, y, z, core: (x, y, z + k, core))


CORE = route(lambda x, y, z, core: (x, y, z, 1 - core))


def move(x, pairs):
    return lax.ppermute(x, BOTH, pairs)


def laplace(cross, left_sq, right_sq, factor):
    v = jnp.maximum(cross + left_sq + right_sq, 1.0)
    return jnp.exp2((v * factor) * lax.rsqrt(v))


def whole(space=pltpu.VMEM):
    return pl.BlockSpec(memory_space=space)


def nn_dot(a, b):
    return jnp.dot(a, b, preferred_element_type=F32)


def upright(row):
    return jnp.broadcast_to(row, (LANES, row.shape[1])).T[:, 0:1]


def score_kernel(factor, sides, fetch, *refs):
    refs = list(refs)
    rows_ref = refs.pop(0)
    side_refs = [tuple(refs.pop(0) for _ in range(3)) for _ in range(sides)]
    fetch_refs = [refs.pop(0) for _ in range(2)] if fetch else []
    start_ref, nys_ref, nys_sq_ref, basis_ref = (None,) * 4 if fetch else (refs.pop(0) for _ in range(4))
    out_ref = refs.pop(0)
    held_refs = [refs.pop(0) for _ in fetch_refs]
    turned = refs.pop(0)
    copies = [pltpu.make_async_copy(a, b, refs[0].at[i]) for i, (a, b) in enumerate(zip(fetch_refs, held_refs))]
    for copy in copies:
        copy.start()
    count = rows_ref.shape[0]
    flat = rows_ref[...].astype(F32).T
    row_sq = jnp.sum(flat * flat, axis=0, keepdims=True)
    turned[...] = (flat * -2.0).astype(BF16)
    jobs = [(*side, slice(at, at + TILE)) for side in side_refs for at in range(0, side[0].shape[0], TILE)]
    cross = nn_dot(jobs[0][0][jobs[0][3], :], turned[...])
    total = jnp.zeros((LANES, count), F32) if fetch else start_ref[...]
    for i, (_, w_ref, sq_ref, at) in enumerate(jobs):
        ahead = None
        if i + 1 < len(jobs):
            centre_ref, _, _, next_at = jobs[i + 1]
            ahead = nn_dot(centre_ref[next_at, :], turned[...])
        kernel = laplace(cross, upright(sq_ref[:, at]), row_sq, factor).astype(BF16)
        total = total + nn_dot(w_ref[:, at], kernel)
        cross = ahead
    if fetch:
        out_ref[...] = total
    else:
        kernel = laplace(nn_dot(nys_ref[...], turned[...]), upright(nys_sq_ref[...]), row_sq, factor)
        basis = lax.dot_general(
            basis_ref[...], kernel, (((0,), (0,)), ((), ())), precision=HIGHEST, preferred_element_type=F32
        )
        out_ref[:, 0:LANES] = total.T.astype(BF16)
        out_ref[:, LANES : 2 * LANES] = basis.T.astype(BF16)
    for copy in copies:
        copy.wait()


def score(factor, rows, sides, fetch=(), rest=()):
    count, dim = rows.shape
    pairs = count * sum(side[0].shape[0] for side in sides)
    out_shape = [jax.ShapeDtypeStruct((LANES, count), F32) if fetch else jax.ShapeDtypeStruct((count, 2 * LANES), BF16)]
    out_shape += [jax.ShapeDtypeStruct(f.shape, f.dtype) for f in fetch]
    flat = [a for side in sides for a in side]
    return pl.pallas_call(
        functools.partial(score_kernel, factor, len(sides), bool(fetch)),
        in_specs=[whole()] * (1 + len(flat)) + [whole(pl.ANY)] * len(fetch) + [whole()] * len(rest),
        out_specs=[whole()] * len(out_shape),
        out_shape=out_shape,
        scratch_shapes=[pltpu.VMEM((dim, count), BF16)] + ([pltpu.SemaphoreType.DMA((2,))] if fetch else []),
        cost_estimate=pl.CostEstimate(flops=2 * pairs * (dim + LANES), bytes_accessed=pairs, transcendentals=2 * pairs),
        compiler_params=pltpu.CompilerParams(vmem_limit_bytes=16 * 1024 * 1024),
    )(rows, *flat, *fetch, *rest)


def pick_kernel(batch_ref, nys_ref, centres_ref, batch_out, nys_out, held, sems):
    copies = []
    count = nys_out.shape[0]
    row = lax.broadcasted_iota(jnp.int32, (2 * count, 16 * count), 0)
    column = lax.broadcasted_iota(jnp.int32, (2 * count, 16 * count), 1)
    target = jnp.zeros_like(column)
    for r in range(2 * count):
        index = batch_ref[r] if r < count else nys_ref[r - count]
        start = pl.multiple_of((index // 8) * 8, 8)
        copy = pltpu.make_async_copy(centres_ref.at[pl.ds(start, 8), :], held.at[pl.ds(8 * r, 8), :], sems.at[r])
        copy.start()
        copies.append(copy)
        target = jnp.where(row == r, 8 * r + (index & 7), target)
    for copy in copies:
        copy.wait()
    chosen = (column == target).astype(F32).astype(BF16)
    rows = jnp.dot(chosen, held[...], preferred_element_type=F32).astype(BF16)
    for i in range(batch_out.shape[0]):
        batch_out[i] = rows[:count]
    nys_out[...] = rows[count:]


def pick_rows(batch_index, nys_index, centres, copies):
    count, dim = batch_index.shape[0], centres.shape[1]
    return pl.pallas_call(
        pick_kernel,
        in_specs=[whole(pltpu.SMEM), whole(pltpu.SMEM), whole(pl.ANY)],
        out_specs=[whole(), whole()],
        out_shape=[jax.ShapeDtypeStruct((copies, count, dim), BF16), jax.ShapeDtypeStruct((count, dim), BF16)],
        scratch_shapes=[pltpu.VMEM((16 * count, dim), BF16), pltpu.SemaphoreType.DMA((2 * count,))],
    )(batch_index, nys_index, centres)


def spread_kernel(*refs):
    out_ref = refs[-1]
    value = refs[0][...]
    for ref in refs[1:-1]:
        value = value + ref[...]
    value = value.astype(BF16)
    for i in range(out_ref.shape[0]):
        out_ref[i] = value


def spread(copies, *arrays):
    return pl.pallas_call(
        spread_kernel,
        in_specs=[whole()] * len(arrays),
        out_specs=whole(),
        out_shape=jax.ShapeDtypeStruct((copies, *arrays[0].shape), BF16),
        compiler_params=pltpu.CompilerParams(vmem_limit_bytes=8 * 1024 * 1024),
    )(*arrays)


def line_kernel(z_ref, parts_ref, targets_ref, out_ref):
    outputs, own = targets_ref.shape
    copies, count = out_ref.shape[0], out_ref.shape[1]
    total = parts_ref[0]
    for i in range(1, parts_ref.shape[0]):
        total = total + parts_ref[i]
    padded = jnp.concatenate([targets_ref[...], jnp.zeros((LANES - outputs, own), F32)], axis=0)
    padded = jnp.concatenate([padded] * (LANES // own), axis=1).T
    row = lax.broadcasted_iota(jnp.int32, (count, LANES), 0)
    mine = (row >= z_ref[0] * own) & (row < z_ref[0] * own + own)
    left = (total[:, :LANES] - jnp.where(mine, padded, 0.0)).astype(BF16)
    right = total[:, LANES:].astype(BF16)
    for i in range(copies):
        out_ref[i, :, 0:LANES] = left
        out_ref[i, :, LANES : 2 * LANES] = right


def line_sum(z, parts, targets, copies):
    return pl.pallas_call(
        line_kernel,
        in_specs=[whole(pltpu.SMEM), whole(), whole()],
        out_specs=whole(),
        out_shape=jax.ShapeDtypeStruct((copies, parts.shape[1], parts.shape[2]), BF16),
        compiler_params=pltpu.CompilerParams(vmem_limit_bytes=8 * 1024 * 1024),
    )(z, parts, targets)


def product_kernel(z_ref, parts_ref, part_ref, rows_ref, held):
    own = rows_ref.shape[0]
    total = parts_ref[0].astype(F32)
    for i in range(1, parts_ref.shape[0]):
        total = total + parts_ref[i].astype(F32)
    residual = total[:, :LANES]
    held[...] = residual
    part_ref[...] = lax.dot_general(
        total[:, LANES:], residual, (((0,), (0,)), ((), ())), precision=HIGHEST, preferred_element_type=F32
    )
    rows_ref[...] = held[pl.ds(pl.multiple_of(z_ref[0] * own, own), own), :]


def product(z, parts, own):
    return pl.pallas_call(
        product_kernel,
        in_specs=[whole(pltpu.SMEM), whole()],
        out_specs=[whole(), whole()],
        out_shape=[jax.ShapeDtypeStruct((LANES, LANES), F32), jax.ShapeDtypeStruct((own, LANES), F32)],
        scratch_shapes=[pltpu.VMEM((parts.shape[1], LANES), F32)],
        compiler_params=pltpu.CompilerParams(vmem_limit_bytes=8 * 1024 * 1024),
    )(z, parts)


Z_GROUPS = [[place(x, y, z, core) for z in range(NZ)] for x in range(NX) for y in range(NY) for core in range(2)]
PLANE_GROUPS = [[place(x, y, z, core) for x in range(NX) for y in range(NY)] for z in range(NZ) for core in range(2)]
FIRST_GROUPS = [[place(i, y, z, 0) for i in range(NX)] for y in range(NY) for z in range(NZ)] + [
    [place(x, i, z, 1) for i in range(NY)] for x in range(NX) for z in range(NZ)
]


def exchange(blocks, groups):
    return lax.all_to_all(blocks, BOTH, split_axis=0, concat_axis=0, tiled=True, axis_index_groups=groups)


def squares(rows):
    return jnp.sum(jnp.square(rows.astype(F32)), axis=1)[None, :]


def per_device(centres, coefficients, targets, batch_index, nys_index, eigvecs, eig_scale):
    own_centres, dim = centres.shape
    outputs = coefficients.shape[0]
    own_batch = targets.shape[1]
    own_nys = nys_index.shape[0]
    factor = -math.log2(math.e) / (0.7 * math.sqrt(dim))
    dev, grp = lax.axis_index("dev"), lax.axis_index("grp")
    z = (((dev >> 2) & 1) * 4 + (grp >> 1))[None]

    peer_centres = move(centres, CORE)
    own_copies, nys_rows = pick_rows(batch_index, nys_index, centres, NZ)
    own_copies, nys_rows, late_coefficients, late_centres = lax.optimization_barrier(
        (own_copies, nys_rows, coefficients, centres)
    )

    line = exchange(own_copies, Z_GROUPS).reshape(NZ * own_batch, dim)
    sheet = exchange(spread(NX, line), FIRST_GROUPS).reshape(NX * NZ * own_batch, dim)
    shifts = (3, 1, 2)
    groups = [move(sheet, plane_route(0, -b)) for b in shifts]

    weights = jnp.pad(late_coefficients.astype(BF16), ((0, LANES - outputs), (0, 0)))
    centre_sq = squares(late_centres)
    peer_weights = move(weights, CORE)
    peer_sq = move(centre_sq, CORE)
    nys_all = jnp.concatenate([nys_rows, move(nys_rows, CORE)], axis=0)
    nys_sq = squares(nys_all)
    basis = jnp.concatenate([eigvecs, move(eigvecs, CORE)], axis=0)

    own_side = (centres, weights, centre_sq)
    own_start, peer_centres, peer_weights = score(factor, sheet, [own_side], fetch=(peer_centres, peer_weights))
    peer_side = (peer_centres, peer_weights, peer_sq)
    nothing = jnp.zeros_like(own_start)
    returned = []
    for b, rows in zip(shifts, groups):
        (part,) = score(factor, rows, [own_side, peer_side], rest=(nothing, nys_all, nys_sq, basis))
        returned.append(move(part, plane_route(0, b)))
    sheet, own_start, *_ = lax.optimization_barrier((sheet, own_start, part))
    (part,) = score(factor, sheet, [peer_side], rest=(own_start, nys_all, nys_sq, basis))
    returned = [part, *returned]
    sheet_sum = functools.reduce(lambda s, r: s + r.astype(F32), returned[1:], returned[0].astype(F32))

    parts = exchange(sheet_sum.reshape(NX, NZ * own_batch, 2 * LANES), FIRST_GROUPS)
    lines = exchange(line_sum(z, parts, targets, NZ), Z_GROUPS)
    part, residual_rows = product(z, lines, own_batch)
    residual_rows = residual_rows[:, :outputs]
    residual_own = residual_rows.T

    parts = exchange(spread(NX * NY, part, move(part, CORE)), PLANE_GROUPS)
    projected = jnp.sum(parts.astype(F32), axis=0)[:, :outputs]
    correction = jnp.dot(eigvecs, eig_scale[:, None] * projected, precision=HIGHEST)

    columns = lax.broadcasted_iota(jnp.int32, (own_batch + own_nys, own_centres), 1)
    chosen = (jnp.concatenate([batch_index, nys_index])[:, None] == columns).astype(F32)
    change = jnp.concatenate([-step_rate * residual_rows, step_rate * correction], axis=0)
    updated = coefficients + lax.dot_general(change, chosen, (((0,), (0,)), ((), ())), precision=HIGHEST)
    return (updated, residual_own)


def solution(mesh):
    in_specs = (
        P(BOTH, None),
        P(None, BOTH),
        P(None, BOTH),
        P(BOTH),
        P(BOTH),
        P(BOTH, None),
        P(),
    )
    out_specs = (P(None, BOTH), P(None, BOTH))
    return jax.shard_map(per_device, mesh=mesh, in_specs=in_specs, out_specs=out_specs, check_vma=False)
```

```python
import functools
import math

import jax
import jax.numpy as jnp
from jax import lax
from jax.experimental import pallas as pl
from jax.experimental.pallas import tpu as pltpu
from jax.sharding import PartitionSpec as P


step_rate = 1.0
LANES = 128
TILE = 1024
BOTH = ("grp", "dev")
F32 = jnp.float32
BF16 = jnp.bfloat16
HIGHEST = lax.Precision.HIGHEST

NX, NY, NZ = 4, 4, 8


def place(x, y, z, core):
    return ((z % 4) * 2 + core) * 32 + x * 8 + (z // 4) * 4 + y


def route(target):
    pairs = []
    for x in range(NX):
        for y in range(NY):
            for z in range(NZ):
                for core in range(2):
                    tx, ty, tz, tc = target(x, y, z, core)
                    pairs.append((place(x, y, z, core), place(tx % NX, ty % NY, tz % NZ, tc)))
    return pairs


def second_route(k):
    return route(lambda x, y, z, core: (x, y ^ k, z, core) if core == 0 else (x ^ k, y, z, core))


CORE = route(lambda x, y, z, core: (x, y, z, 1 - core))


def move(x, pairs):
    return lax.ppermute(x, BOTH, pairs)


def laplace(cross, left_sq, right_sq, factor):
    v = jnp.maximum(cross + left_sq + right_sq, 1.0)
    return jnp.exp2((v * factor) * lax.rsqrt(v))


def whole(space=pltpu.VMEM):
    return pl.BlockSpec(memory_space=space)


def nn_dot(a, b):
    return jnp.dot(a, b, preferred_element_type=F32)


def upright(row):
    return jnp.broadcast_to(row, (LANES, row.shape[1])).T[:, 0:1]


def score_kernel(factor, sides, fetch, *refs):
    refs = list(refs)
    rows_ref = refs.pop(0)
    side_refs = [tuple(refs.pop(0) for _ in range(3)) for _ in range(sides)]
    fetch_refs = [refs.pop(0) for _ in range(2)] if fetch else []
    start_ref, nys_ref, nys_sq_ref, basis_ref = (None,) * 4 if fetch else (refs.pop(0) for _ in range(4))
    out_ref = refs.pop(0)
    held_refs = [refs.pop(0) for _ in fetch_refs]
    turned = refs.pop(0)
    copies = [pltpu.make_async_copy(a, b, refs[0].at[i]) for i, (a, b) in enumerate(zip(fetch_refs, held_refs))]
    for copy in copies:
        copy.start()
    count = rows_ref.shape[0]
    flat = rows_ref[...].T.astype(F32)
    row_sq = jnp.sum(flat * flat, axis=0, keepdims=True)
    turned[...] = (flat * -2.0).astype(BF16)
    jobs = [(*side, slice(at, at + TILE)) for side in side_refs for at in range(0, side[0].shape[0], TILE)]
    cross = nn_dot(jobs[0][0][jobs[0][3], :], turned[...])
    total = jnp.zeros((LANES, count), F32) if fetch else start_ref[...]
    for i, (_, w_ref, sq_ref, at) in enumerate(jobs):
        ahead = None
        if i + 1 < len(jobs):
            centre_ref, _, _, next_at = jobs[i + 1]
            ahead = nn_dot(centre_ref[next_at, :], turned[...])
        column = upright(sq_ref[:, at])
        lanes = [slice(c, c + count // 2) for c in (0, count // 2)]
        kernel = jnp.concatenate(
            [laplace(cross[:, c], column, row_sq[:, c], factor).astype(BF16) for c in lanes], axis=1
        )
        total = total + nn_dot(w_ref[:, at], kernel)
        cross = ahead
    if fetch:
        out_ref[...] = total
    else:
        kernel = laplace(nn_dot(nys_ref[...], turned[...]), upright(nys_sq_ref[...]), row_sq, factor)
        basis = lax.dot_general(
            basis_ref[...], kernel, (((0,), (0,)), ((), ())), precision=HIGHEST, preferred_element_type=F32
        )
        out_ref[:, 0:LANES] = total.T.astype(BF16)
        out_ref[:, LANES : 2 * LANES] = basis.T.astype(BF16)
    for copy in copies:
        copy.wait()


def score(factor, rows, sides, fetch=(), rest=()):
    count, dim = rows.shape
    pairs = count * sum(side[0].shape[0] for side in sides)
    out_shape = [jax.ShapeDtypeStruct((LANES, count), F32) if fetch else jax.ShapeDtypeStruct((count, 2 * LANES), BF16)]
    out_shape += [jax.ShapeDtypeStruct(f.shape, f.dtype) for f in fetch]
    flat = [a for side in sides for a in side]
    return pl.pallas_call(
        functools.partial(score_kernel, factor, len(sides), bool(fetch)),
        in_specs=[whole()] * (1 + len(flat)) + [whole(pl.ANY)] * len(fetch) + [whole()] * len(rest),
        out_specs=[whole()] * len(out_shape),
        out_shape=out_shape,
        scratch_shapes=[pltpu.VMEM((dim, count), BF16)] + ([pltpu.SemaphoreType.DMA((2,))] if fetch else []),
        cost_estimate=pl.CostEstimate(flops=2 * pairs * (dim + LANES), bytes_accessed=pairs, transcendentals=2 * pairs),
        compiler_params=pltpu.CompilerParams(vmem_limit_bytes=16 * 1024 * 1024),
    )(rows, *flat, *fetch, *rest)


def pick_kernel(batch_ref, nys_ref, centres_ref, batch_out, nys_out, held, sems):
    copies = []
    count = nys_out.shape[0]
    row = lax.broadcasted_iota(jnp.int32, (2 * count, 16 * count), 0)
    column = lax.broadcasted_iota(jnp.int32, (2 * count, 16 * count), 1)
    target = jnp.zeros_like(column)
    for r in range(2 * count):
        index = batch_ref[r] if r < count else nys_ref[r - count]
        start = pl.multiple_of((index // 8) * 8, 8)
        copy = pltpu.make_async_copy(centres_ref.at[pl.ds(start, 8), :], held.at[pl.ds(8 * r, 8), :], sems.at[r])
        copy.start()
        copies.append(copy)
        target = jnp.where(row == r, 8 * r + (index & 7), target)
    for copy in copies:
        copy.wait()
    chosen = (column == target).astype(F32).astype(BF16)
    rows = jnp.dot(chosen, held[...], preferred_element_type=F32).astype(BF16)
    for i in range(batch_out.shape[0]):
        batch_out[i] = rows[:count]
    nys_out[...] = rows[count:]


def pick_rows(batch_index, nys_index, centres, copies):
    count, dim = batch_index.shape[0], centres.shape[1]
    return pl.pallas_call(
        pick_kernel,
        in_specs=[whole(pltpu.SMEM), whole(pltpu.SMEM), whole(pl.ANY)],
        out_specs=[whole(), whole()],
        out_shape=[jax.ShapeDtypeStruct((copies, count, dim), BF16), jax.ShapeDtypeStruct((count, dim), BF16)],
        scratch_shapes=[pltpu.VMEM((16 * count, dim), BF16), pltpu.SemaphoreType.DMA((2 * count,))],
    )(batch_index, nys_index, centres)


def spread_kernel(*refs):
    out_ref = refs[-1]
    value = refs[0][...]
    for ref in refs[1:-1]:
        value = value + ref[...]
    value = value.astype(BF16)
    for i in range(out_ref.shape[0]):
        out_ref[i] = value


def spread(copies, *arrays):
    return pl.pallas_call(
        spread_kernel,
        in_specs=[whole()] * len(arrays),
        out_specs=whole(),
        out_shape=jax.ShapeDtypeStruct((copies, *arrays[0].shape), BF16),
        compiler_params=pltpu.CompilerParams(vmem_limit_bytes=8 * 1024 * 1024),
    )(*arrays)


def line_kernel(z_ref, parts_ref, targets_ref, out_ref):
    outputs, own = targets_ref.shape
    copies, count = out_ref.shape[0], out_ref.shape[1]
    total = parts_ref[0]
    for i in range(1, parts_ref.shape[0]):
        total = total + parts_ref[i]
    padded = jnp.concatenate([targets_ref[...], jnp.zeros((LANES - outputs, own), F32)], axis=0)
    padded = jnp.concatenate([padded] * (LANES // own), axis=1).T
    row = lax.broadcasted_iota(jnp.int32, (count, LANES), 0)
    mine = (row >= z_ref[0] * own) & (row < z_ref[0] * own + own)
    left = (total[:, :LANES] - jnp.where(mine, padded, 0.0)).astype(BF16)
    right = total[:, LANES:].astype(BF16)
    for i in range(copies):
        out_ref[i, :, 0:LANES] = left
        out_ref[i, :, LANES : 2 * LANES] = right


def line_sum(z, parts, targets, copies):
    return pl.pallas_call(
        line_kernel,
        in_specs=[whole(pltpu.SMEM), whole(), whole()],
        out_specs=whole(),
        out_shape=jax.ShapeDtypeStruct((copies, parts.shape[1], parts.shape[2]), BF16),
        compiler_params=pltpu.CompilerParams(vmem_limit_bytes=8 * 1024 * 1024),
    )(z, parts, targets)


def product_kernel(z_ref, parts_ref, part_ref, rows_ref, held):
    own = rows_ref.shape[0]
    total = parts_ref[0].astype(F32)
    for i in range(1, parts_ref.shape[0]):
        total = total + parts_ref[i].astype(F32)
    residual = total[:, :LANES]
    held[...] = residual
    part_ref[...] = lax.dot_general(
        total[:, LANES:], residual, (((0,), (0,)), ((), ())), precision=HIGHEST, preferred_element_type=F32
    )
    rows_ref[...] = held[pl.ds(pl.multiple_of(z_ref[0] * own, own), own), :]


def product(z, parts, own):
    return pl.pallas_call(
        product_kernel,
        in_specs=[whole(pltpu.SMEM), whole()],
        out_specs=[whole(), whole()],
        out_shape=[jax.ShapeDtypeStruct((LANES, LANES), F32), jax.ShapeDtypeStruct((own, LANES), F32)],
        scratch_shapes=[pltpu.VMEM((parts.shape[1], LANES), F32)],
        compiler_params=pltpu.CompilerParams(vmem_limit_bytes=8 * 1024 * 1024),
    )(z, parts)


Z_GROUPS = [[place(x, y, z, core) for z in range(NZ)] for x in range(NX) for y in range(NY) for core in range(2)]
PLANE_GROUPS = [[place(x, y, z, core) for x in range(NX) for y in range(NY)] for z in range(NZ) for core in range(2)]
FIRST_GROUPS = [[place(i, y, z, 0) for i in range(NX)] for y in range(NY) for z in range(NZ)] + [
    [place(x, i, z, 1) for i in range(NY)] for x in range(NX) for z in range(NZ)
]


def exchange(blocks, groups):
    return lax.all_to_all(blocks, BOTH, split_axis=0, concat_axis=0, tiled=True, axis_index_groups=groups)


def squares(rows):
    return jnp.sum(jnp.square(rows.astype(F32)), axis=1)[None, :]


def per_device(centres, coefficients, targets, batch_index, nys_index, eigvecs, eig_scale):
    own_centres, dim = centres.shape
    outputs = coefficients.shape[0]
    own_batch = targets.shape[1]
    own_nys = nys_index.shape[0]
    factor = -math.log2(math.e) / (0.7 * math.sqrt(dim))
    dev, grp = lax.axis_index("dev"), lax.axis_index("grp")
    z = (((dev >> 2) & 1) * 4 + (grp >> 1))[None]

    peer_centres = move(centres, CORE)
    own_copies, nys_rows = pick_rows(batch_index, nys_index, centres, NZ)
    own_copies, nys_rows, late_coefficients, late_centres = lax.optimization_barrier(
        (own_copies, nys_rows, coefficients, centres)
    )

    line = exchange(own_copies, Z_GROUPS).reshape(NZ * own_batch, dim)
    sheet = exchange(spread(NX, line), FIRST_GROUPS).reshape(NX * NZ * own_batch, dim)
    shifts = (1, 2, 3)
    groups = [move(sheet, second_route(b)) for b in shifts]

    weights = jnp.pad(late_coefficients.astype(BF16), ((0, LANES - outputs), (0, 0)))
    centre_sq = squares(late_centres)
    peer_weights = move(weights, CORE)
    peer_sq = move(centre_sq, CORE)
    nys_all = jnp.concatenate([nys_rows, move(nys_rows, CORE)], axis=0)
    nys_sq = squares(nys_all)
    basis = jnp.concatenate([eigvecs, move(eigvecs, CORE)], axis=0)

    own_side = (centres, weights, centre_sq)
    own_start, peer_centres, peer_weights = score(factor, sheet, [own_side], fetch=(peer_centres, peer_weights))
    peer_side = (peer_centres, peer_weights, peer_sq)
    nothing = jnp.zeros_like(own_start)
    returned = []
    for b, rows in zip(shifts, groups):
        (part,) = score(factor, rows, [own_side, peer_side], rest=(nothing, nys_all, nys_sq, basis))
        returned.append(move(part, second_route(b)))
    sheet, own_start, *_ = lax.optimization_barrier((sheet, own_start, part))
    (part,) = score(factor, sheet, [peer_side], rest=(own_start, nys_all, nys_sq, basis))
    returned = [part, *returned]
    sheet_sum = functools.reduce(lambda s, r: s + r.astype(F32), returned[1:], returned[0].astype(F32))

    parts = exchange(sheet_sum.reshape(NX, NZ * own_batch, 2 * LANES), FIRST_GROUPS)
    lines = exchange(line_sum(z, parts, targets, NZ), Z_GROUPS)
    part, residual_rows = product(z, lines, own_batch)
    residual_rows = residual_rows[:, :outputs]
    residual_own = residual_rows.T

    parts = exchange(spread(NX * NY, part, move(part, CORE)), PLANE_GROUPS)
    projected = jnp.sum(parts.astype(F32), axis=0)[:, :outputs]
    correction = jnp.dot(eigvecs, eig_scale[:, None] * projected, precision=HIGHEST)

    columns = lax.broadcasted_iota(jnp.int32, (own_batch + own_nys, own_centres), 1)
    chosen = (jnp.concatenate([batch_index, nys_index])[:, None] == columns).astype(F32)
    change = jnp.concatenate([-step_rate * residual_rows, step_rate * correction], axis=0)
    updated = coefficients + lax.dot_general(change, chosen, (((0,), (0,)), ((), ())), precision=HIGHEST)
    return (updated, residual_own)


def solution(mesh):
    in_specs = (
        P(BOTH, None),
        P(None, BOTH),
        P(None, BOTH),
        P(BOTH),
        P(BOTH),
        P(BOTH, None),
        P(),
    )
    out_specs = (P(None, BOTH), P(None, BOTH))
    return jax.shard_map(per_device, mesh=mesh, in_specs=in_specs, out_specs=out_specs, check_vma=False)
```

```python
import functools
import math

import jax
import jax.numpy as jnp
from jax import lax
from jax.experimental import pallas as pl
from jax.experimental.pallas import tpu as pltpu
from jax.sharding import PartitionSpec as P


step_rate = 1.0
LANES = 128
TILE = 1024
BOTH = ("grp", "dev")
F32 = jnp.float32
BF16 = jnp.bfloat16
HIGHEST = lax.Precision.HIGHEST

NX, NY, NZ = 4, 4, 8


def place(x, y, z, core):
    return ((z % 4) * 2 + core) * 32 + x * 8 + (z // 4) * 4 + y


def route(target):
    pairs = []
    for x in range(NX):
        for y in range(NY):
            for z in range(NZ):
                for core in range(2):
                    tx, ty, tz, tc = target(x, y, z, core)
                    pairs.append((place(x, y, z, core), place(tx % NX, ty % NY, tz % NZ, tc)))
    return pairs


def second_route(k):
    return route(lambda x, y, z, core: (x, y ^ k, z, core) if core == 0 else (x ^ k, y, z, core))


CORE = route(lambda x, y, z, core: (x, y, z, 1 - core))


def move(x, pairs):
    return lax.ppermute(x, BOTH, pairs)


def laplace(cross, left_sq, right_sq, factor):
    v = jnp.maximum(cross + left_sq + right_sq, 1.0)
    return jnp.exp2((v * factor) * lax.rsqrt(v))


def whole(space=pltpu.VMEM):
    return pl.BlockSpec(memory_space=space)


def nn_dot(a, b):
    return jnp.dot(a, b, preferred_element_type=F32)


def upright(row):
    return jnp.broadcast_to(row, (LANES, row.shape[1])).T[:, 0:1]


def score_kernel(factor, sides, fetch, *refs):
    refs = list(refs)
    rows_ref = refs.pop(0)
    side_refs = [tuple(refs.pop(0) for _ in range(3)) for _ in range(sides)]
    fetch_refs = [refs.pop(0) for _ in range(2)] if fetch else []
    start_ref, nys_ref, nys_sq_ref, basis_ref = (None,) * 4 if fetch else (refs.pop(0) for _ in range(4))
    out_ref = refs.pop(0)
    held_refs = [refs.pop(0) for _ in fetch_refs]
    turned = refs.pop(0)
    copies = [pltpu.make_async_copy(a, b, refs[0].at[i]) for i, (a, b) in enumerate(zip(fetch_refs, held_refs))]
    for copy in copies:
        copy.start()
    count = rows_ref.shape[0]
    flat = rows_ref[...].T.astype(F32)
    row_sq = jnp.sum(flat * flat, axis=0, keepdims=True)
    turned[...] = (flat * -2.0).astype(BF16)
    jobs = [(*side, slice(at, at + TILE)) for side in side_refs for at in range(0, side[0].shape[0], TILE)]
    cross = nn_dot(jobs[0][0][jobs[0][3], :], turned[...])
    total = jnp.zeros((LANES, count), F32) if fetch else start_ref[...]
    for i, (_, w_ref, sq_ref, at) in enumerate(jobs):
        ahead = None
        if i + 1 < len(jobs):
            centre_ref, _, _, next_at = jobs[i + 1]
            ahead = nn_dot(centre_ref[next_at, :], turned[...])
        column = upright(sq_ref[:, at])
        lanes = [slice(c, c + count // 2) for c in (0, count // 2)]
        kernel = jnp.concatenate(
            [laplace(cross[:, c], column, row_sq[:, c], factor).astype(BF16) for c in lanes], axis=1
        )
        total = total + nn_dot(w_ref[:, at], kernel)
        cross = ahead
    if fetch:
        out_ref[...] = total
    else:
        kernel = laplace(nn_dot(nys_ref[...], turned[...]), upright(nys_sq_ref[...]), row_sq, factor)
        basis = lax.dot_general(
            basis_ref[...], kernel, (((0,), (0,)), ((), ())), precision=HIGHEST, preferred_element_type=F32
        )
        out_ref[:, 0:LANES] = total.T.astype(BF16)
        out_ref[:, LANES : 2 * LANES] = basis.T.astype(BF16)
    for copy in copies:
        copy.wait()


def score(factor, rows, sides, fetch=(), rest=()):
    count, dim = rows.shape
    pairs = count * sum(side[0].shape[0] for side in sides)
    out_shape = [jax.ShapeDtypeStruct((LANES, count), F32) if fetch else jax.ShapeDtypeStruct((count, 2 * LANES), BF16)]
    out_shape += [jax.ShapeDtypeStruct(f.shape, f.dtype) for f in fetch]
    flat = [a for side in sides for a in side]
    return pl.pallas_call(
        functools.partial(score_kernel, factor, len(sides), bool(fetch)),
        in_specs=[whole()] * (1 + len(flat)) + [whole(pl.ANY)] * len(fetch) + [whole()] * len(rest),
        out_specs=[whole()] * len(out_shape),
        out_shape=out_shape,
        scratch_shapes=[pltpu.VMEM((dim, count), BF16)] + ([pltpu.SemaphoreType.DMA((2,))] if fetch else []),
        cost_estimate=pl.CostEstimate(flops=2 * pairs * (dim + LANES), bytes_accessed=pairs, transcendentals=2 * pairs),
        compiler_params=pltpu.CompilerParams(vmem_limit_bytes=16 * 1024 * 1024),
    )(rows, *flat, *fetch, *rest)


def pick_kernel(batch_ref, nys_ref, centres_ref, batch_out, nys_out, held, sems):
    copies = []
    count = nys_out.shape[0]
    row = lax.broadcasted_iota(jnp.int32, (2 * count, 16 * count), 0)
    column = lax.broadcasted_iota(jnp.int32, (2 * count, 16 * count), 1)
    target = jnp.zeros_like(column)
    for r in range(2 * count):
        index = batch_ref[r] if r < count else nys_ref[r - count]
        start = pl.multiple_of((index // 8) * 8, 8)
        copy = pltpu.make_async_copy(centres_ref.at[pl.ds(start, 8), :], held.at[pl.ds(8 * r, 8), :], sems.at[r])
        copy.start()
        copies.append(copy)
        target = jnp.where(row == r, 8 * r + (index & 7), target)
    for copy in copies:
        copy.wait()
    chosen = (column == target).astype(F32).astype(BF16)
    rows = jnp.dot(chosen, held[...], preferred_element_type=F32).astype(BF16)
    for i in range(batch_out.shape[0]):
        batch_out[i] = rows[:count]
    nys_out[...] = rows[count:]


def pick_rows(batch_index, nys_index, centres, copies):
    count, dim = batch_index.shape[0], centres.shape[1]
    return pl.pallas_call(
        pick_kernel,
        in_specs=[whole(pltpu.SMEM), whole(pltpu.SMEM), whole(pl.ANY)],
        out_specs=[whole(), whole()],
        out_shape=[jax.ShapeDtypeStruct((copies, count, dim), BF16), jax.ShapeDtypeStruct((count, dim), BF16)],
        scratch_shapes=[pltpu.VMEM((16 * count, dim), BF16), pltpu.SemaphoreType.DMA((2 * count,))],
    )(batch_index, nys_index, centres)


def spread_kernel(*refs):
    out_ref = refs[-1]
    value = refs[0][...]
    for ref in refs[1:-1]:
        value = value + ref[...]
    value = value.astype(BF16)
    for i in range(out_ref.shape[0]):
        out_ref[i] = value


def spread(copies, *arrays):
    return pl.pallas_call(
        spread_kernel,
        in_specs=[whole()] * len(arrays),
        out_specs=whole(),
        out_shape=jax.ShapeDtypeStruct((copies, *arrays[0].shape), BF16),
        compiler_params=pltpu.CompilerParams(vmem_limit_bytes=8 * 1024 * 1024),
    )(*arrays)


def line_kernel(z_ref, parts_ref, targets_ref, out_ref):
    outputs, own = targets_ref.shape
    copies, count = out_ref.shape[0], out_ref.shape[1]
    total = parts_ref[0].astype(F32)
    for i in range(1, parts_ref.shape[0]):
        total = total + parts_ref[i].astype(F32)
    padded = jnp.concatenate([targets_ref[...], jnp.zeros((LANES - outputs, own), F32)], axis=0)
    padded = jnp.concatenate([padded] * (LANES // own), axis=1).T
    row = lax.broadcasted_iota(jnp.int32, (count, LANES), 0)
    mine = (row >= z_ref[0] * own) & (row < z_ref[0] * own + own)
    left = (total[:, :LANES] - jnp.where(mine, padded, 0.0)).astype(BF16)
    right = total[:, LANES:].astype(BF16)
    for i in range(copies):
        out_ref[i, :, 0:LANES] = left
        out_ref[i, :, LANES : 2 * LANES] = right


def line_sum(z, parts, targets, copies):
    return pl.pallas_call(
        line_kernel,
        in_specs=[whole(pltpu.SMEM), whole(), whole()],
        out_specs=whole(),
        out_shape=jax.ShapeDtypeStruct((copies, parts.shape[1], parts.shape[2]), BF16),
        compiler_params=pltpu.CompilerParams(vmem_limit_bytes=8 * 1024 * 1024),
    )(z, parts, targets)


def product_kernel(z_ref, parts_ref, part_ref, rows_ref, held):
    own = rows_ref.shape[0]
    total = parts_ref[0].astype(F32)
    for i in range(1, parts_ref.shape[0]):
        total = total + parts_ref[i].astype(F32)
    residual = total[:, :LANES]
    held[...] = residual
    part_ref[...] = lax.dot_general(
        total[:, LANES:], residual, (((0,), (0,)), ((), ())), precision=HIGHEST, preferred_element_type=F32
    )
    rows_ref[...] = held[pl.ds(pl.multiple_of(z_ref[0] * own, own), own), :]


def product(z, parts, own):
    return pl.pallas_call(
        product_kernel,
        in_specs=[whole(pltpu.SMEM), whole()],
        out_specs=[whole(), whole()],
        out_shape=[jax.ShapeDtypeStruct((LANES, LANES), F32), jax.ShapeDtypeStruct((own, LANES), F32)],
        scratch_shapes=[pltpu.VMEM((parts.shape[1], LANES), F32)],
        compiler_params=pltpu.CompilerParams(vmem_limit_bytes=8 * 1024 * 1024),
    )(z, parts)


Z_GROUPS = [[place(x, y, z, core) for z in range(NZ)] for x in range(NX) for y in range(NY) for core in range(2)]
PLANE_GROUPS = [[place(x, y, z, core) for x in range(NX) for y in range(NY)] for z in range(NZ) for core in range(2)]
FIRST_GROUPS = [[place(i, y, z, 0) for i in range(NX)] for y in range(NY) for z in range(NZ)] + [
    [place(x, i, z, 1) for i in range(NY)] for x in range(NX) for z in range(NZ)
]


def exchange(blocks, groups):
    return lax.all_to_all(blocks, BOTH, split_axis=0, concat_axis=0, tiled=True, axis_index_groups=groups)


def squares(rows):
    return jnp.sum(jnp.square(rows.astype(F32)), axis=1)[None, :]


def per_device(centres, coefficients, targets, batch_index, nys_index, eigvecs, eig_scale):
    own_centres, dim = centres.shape
    outputs = coefficients.shape[0]
    own_batch = targets.shape[1]
    own_nys = nys_index.shape[0]
    factor = -math.log2(math.e) / (0.7 * math.sqrt(dim))
    dev, grp = lax.axis_index("dev"), lax.axis_index("grp")
    z = (((dev >> 2) & 1) * 4 + (grp >> 1))[None]

    peer_centres = move(centres, CORE)
    own_copies, nys_rows = pick_rows(batch_index, nys_index, centres, NZ)
    own_copies, nys_rows, late_coefficients, late_centres = lax.optimization_barrier(
        (own_copies, nys_rows, coefficients, centres)
    )

    line = exchange(own_copies, Z_GROUPS).reshape(NZ * own_batch, dim)
    sheet = exchange(spread(NX, line), FIRST_GROUPS).reshape(NX * NZ * own_batch, dim)
    shifts = (1, 2, 3)
    groups = [move(sheet, second_route(b)) for b in shifts]

    weights = jnp.pad(late_coefficients.astype(BF16), ((0, LANES - outputs), (0, 0)))
    centre_sq = squares(late_centres)
    peer_weights = move(weights, CORE)
    peer_sq = move(centre_sq, CORE)
    nys_all = jnp.concatenate([nys_rows, move(nys_rows, CORE)], axis=0)
    nys_sq = squares(nys_all)
    basis = jnp.concatenate([eigvecs, move(eigvecs, CORE)], axis=0)

    own_side = (centres, weights, centre_sq)
    own_start, peer_centres, peer_weights = score(factor, sheet, [own_side], fetch=(peer_centres, peer_weights))
    peer_side = (peer_centres, peer_weights, peer_sq)
    nothing = jnp.zeros_like(own_start)
    returned = []
    for b, rows in zip(shifts, groups):
        (part,) = score(factor, rows, [own_side, peer_side], rest=(nothing, nys_all, nys_sq, basis))
        returned.append(move(part, second_route(b)))
    sheet, own_start, *_ = lax.optimization_barrier((sheet, own_start, part))
    (part,) = score(factor, sheet, [peer_side], rest=(own_start, nys_all, nys_sq, basis))
    returned = [part, *returned]
    sheet_sum = functools.reduce(lambda s, r: s + r.astype(F32), returned[1:], returned[0].astype(F32))

    sheet_sum = sheet_sum.astype(BF16)
    parts = exchange(sheet_sum.reshape(NX, NZ * own_batch, 2 * LANES), FIRST_GROUPS)
    lines = exchange(line_sum(z, parts, targets, NZ), Z_GROUPS)
    part, residual_rows = product(z, lines, own_batch)
    residual_rows = residual_rows[:, :outputs]
    residual_own = residual_rows.T

    parts = exchange(spread(NX * NY, part, move(part, CORE)), PLANE_GROUPS)
    projected = jnp.sum(parts.astype(F32), axis=0)[:, :outputs]
    correction = jnp.dot(eigvecs, eig_scale[:, None] * projected, precision=HIGHEST)

    columns = lax.broadcasted_iota(jnp.int32, (own_batch + own_nys, own_centres), 1)
    chosen = (jnp.concatenate([batch_index, nys_index])[:, None] == columns).astype(F32)
    change = jnp.concatenate([-step_rate * residual_rows, step_rate * correction], axis=0)
    updated = coefficients + lax.dot_general(change, chosen, (((0,), (0,)), ((), ())), precision=HIGHEST)
    return (updated, residual_own)


def solution(mesh):
    in_specs = (
        P(BOTH, None),
        P(None, BOTH),
        P(None, BOTH),
        P(BOTH),
        P(BOTH),
        P(BOTH, None),
        P(),
    )
    out_specs = (P(None, BOTH), P(None, BOTH))
    return jax.shard_map(per_device, mesh=mesh, in_specs=in_specs, out_specs=out_specs, check_vma=False)
```

```python
import functools
import math

import jax
import jax.numpy as jnp
from jax import lax
from jax.experimental import pallas as pl
from jax.experimental.pallas import tpu as pltpu
from jax.sharding import PartitionSpec as P


step_rate = 1.0
LANES = 128
TILE = 1024
BOTH = ("grp", "dev")
F32 = jnp.float32
BF16 = jnp.bfloat16
HIGHEST = lax.Precision.HIGHEST

NX, NY, NZ = 4, 4, 8


def place(x, y, z, core):
    return ((z % 4) * 2 + core) * 32 + x * 8 + (z // 4) * 4 + y


def route(target):
    pairs = []
    for x in range(NX):
        for y in range(NY):
            for z in range(NZ):
                for core in range(2):
                    tx, ty, tz, tc = target(x, y, z, core)
                    pairs.append((place(x, y, z, core), place(tx % NX, ty % NY, tz % NZ, tc)))
    return pairs


def second_route(k):
    return route(lambda x, y, z, core: (x, y ^ k, z, core) if core == 0 else (x ^ k, y, z, core))


CORE = route(lambda x, y, z, core: (x, y, z, 1 - core))


def move(x, pairs):
    return lax.ppermute(x, BOTH, pairs)


def laplace(cross, left_sq, right_sq, factor):
    v = jnp.maximum(cross + left_sq + right_sq, 1.0)
    return jnp.exp2((v * factor) * lax.rsqrt(v))


def whole(space=pltpu.VMEM):
    return pl.BlockSpec(memory_space=space)


def nn_dot(a, b):
    return jnp.dot(a, b, preferred_element_type=F32)


def upright(row):
    return jnp.broadcast_to(row, (LANES, row.shape[1])).T[:, 0:1]


def score_kernel(factor, sides, fetch, *refs):
    refs = list(refs)
    rows_ref = refs.pop(0)
    side_refs = [tuple(refs.pop(0) for _ in range(3)) for _ in range(sides)]
    fetch_refs = [refs.pop(0) for _ in range(2)] if fetch else []
    start_ref, nys_ref, nys_sq_ref, basis_ref = (None,) * 4 if fetch else (refs.pop(0) for _ in range(4))
    out_ref = refs.pop(0)
    held_refs = [refs.pop(0) for _ in fetch_refs]
    turned = refs.pop(0)
    copies = [pltpu.make_async_copy(a, b, refs[0].at[i]) for i, (a, b) in enumerate(zip(fetch_refs, held_refs))]
    for copy in copies:
        copy.start()
    count = rows_ref.shape[0]
    flat = rows_ref[...].T.astype(F32)
    row_sq = jnp.sum(flat * flat, axis=0, keepdims=True)
    turned[...] = (flat * -2.0).astype(BF16)
    jobs = [(*side, slice(at, at + TILE)) for side in side_refs for at in range(0, side[0].shape[0], TILE)]
    cross = nn_dot(jobs[0][0][jobs[0][3], :], turned[...])
    total = jnp.zeros((LANES, count), F32) if fetch else start_ref[...]
    for i, (_, w_ref, sq_ref, at) in enumerate(jobs):
        ahead = None
        if i + 1 < len(jobs):
            centre_ref, _, _, next_at = jobs[i + 1]
            ahead = nn_dot(centre_ref[next_at, :], turned[...])
        column = upright(sq_ref[:, at])
        lanes = [slice(c, c + count // 2) for c in (0, count // 2)]
        kernel = jnp.concatenate(
            [laplace(cross[:, c], column, row_sq[:, c], factor).astype(BF16) for c in lanes], axis=1
        )
        total = total + nn_dot(w_ref[:, at], kernel)
        cross = ahead
    if fetch:
        out_ref[...] = total
    else:
        kernel = laplace(nn_dot(nys_ref[...], turned[...]), upright(nys_sq_ref[...]), row_sq, factor)
        basis = lax.dot_general(
            basis_ref[...], kernel, (((0,), (0,)), ((), ())), precision=HIGHEST, preferred_element_type=F32
        )
        out_ref[:, 0:LANES] = total.T.astype(BF16)
        out_ref[:, LANES : 2 * LANES] = basis.T.astype(BF16)
    for copy in copies:
        copy.wait()


def score(factor, rows, sides, fetch=(), rest=()):
    count, dim = rows.shape
    pairs = count * sum(side[0].shape[0] for side in sides)
    out_shape = [jax.ShapeDtypeStruct((LANES, count), F32) if fetch else jax.ShapeDtypeStruct((count, 2 * LANES), BF16)]
    out_shape += [jax.ShapeDtypeStruct(f.shape, f.dtype) for f in fetch]
    flat = [a for side in sides for a in side]
    return pl.pallas_call(
        functools.partial(score_kernel, factor, len(sides), bool(fetch)),
        in_specs=[whole()] * (1 + len(flat)) + [whole(pl.ANY)] * len(fetch) + [whole()] * len(rest),
        out_specs=[whole()] * len(out_shape),
        out_shape=out_shape,
        scratch_shapes=[pltpu.VMEM((dim, count), BF16)] + ([pltpu.SemaphoreType.DMA((2,))] if fetch else []),
        cost_estimate=pl.CostEstimate(flops=2 * pairs * (dim + LANES), bytes_accessed=pairs, transcendentals=2 * pairs),
        compiler_params=pltpu.CompilerParams(vmem_limit_bytes=16 * 1024 * 1024),
    )(rows, *flat, *fetch, *rest)


def pick_kernel(batch_ref, nys_ref, centres_ref, batch_out, nys_out, held, sems):
    copies = []
    count = nys_out.shape[0]
    row = lax.broadcasted_iota(jnp.int32, (2 * count, 16 * count), 0)
    column = lax.broadcasted_iota(jnp.int32, (2 * count, 16 * count), 1)
    target = jnp.zeros_like(column)
    for r in range(2 * count):
        index = batch_ref[r] if r < count else nys_ref[r - count]
        start = pl.multiple_of((index // 8) * 8, 8)
        copy = pltpu.make_async_copy(centres_ref.at[pl.ds(start, 8), :], held.at[pl.ds(8 * r, 8), :], sems.at[r])
        copy.start()
        copies.append(copy)
        target = jnp.where(row == r, 8 * r + (index & 7), target)
    for copy in copies:
        copy.wait()
    chosen = (column == target).astype(F32).astype(BF16)
    rows = jnp.dot(chosen, held[...], preferred_element_type=F32).astype(BF16)
    for i in range(batch_out.shape[0]):
        batch_out[i] = rows[:count]
    nys_out[...] = rows[count:]


def pick_rows(batch_index, nys_index, centres, copies):
    count, dim = batch_index.shape[0], centres.shape[1]
    return pl.pallas_call(
        pick_kernel,
        in_specs=[whole(pltpu.SMEM), whole(pltpu.SMEM), whole(pl.ANY)],
        out_specs=[whole(), whole()],
        out_shape=[jax.ShapeDtypeStruct((copies, count, dim), BF16), jax.ShapeDtypeStruct((count, dim), BF16)],
        scratch_shapes=[pltpu.VMEM((16 * count, dim), BF16), pltpu.SemaphoreType.DMA((2 * count,))],
    )(batch_index, nys_index, centres)


def spread_kernel(*refs):
    out_ref = refs[-1]
    value = refs[0][...]
    for ref in refs[1:-1]:
        value = value + ref[...]
    value = value.astype(BF16)
    for i in range(out_ref.shape[0]):
        out_ref[i] = value


def spread(copies, *arrays):
    return pl.pallas_call(
        spread_kernel,
        in_specs=[whole()] * len(arrays),
        out_specs=whole(),
        out_shape=jax.ShapeDtypeStruct((copies, *arrays[0].shape), BF16),
        compiler_params=pltpu.CompilerParams(vmem_limit_bytes=8 * 1024 * 1024),
    )(*arrays)


def line_kernel(z_ref, parts_ref, targets_ref, out_ref):
    outputs, own = targets_ref.shape
    copies, count = out_ref.shape[0], out_ref.shape[1]
    total = parts_ref[0].astype(F32)
    for i in range(1, parts_ref.shape[0]):
        total = total + parts_ref[i].astype(F32)
    padded = jnp.concatenate([targets_ref[...], jnp.zeros((LANES - outputs, own), F32)], axis=0)
    padded = jnp.concatenate([padded] * (LANES // own), axis=1).T
    row = lax.broadcasted_iota(jnp.int32, (count, LANES), 0)
    mine = (row >= z_ref[0] * own) & (row < z_ref[0] * own + own)
    left = (total[:, :LANES] - jnp.where(mine, padded, 0.0)).astype(BF16)
    right = total[:, LANES:].astype(BF16)
    for i in range(copies):
        out_ref[i, :, 0:LANES] = left
        out_ref[i, :, LANES : 2 * LANES] = right


def line_sum(z, parts, targets, copies):
    return pl.pallas_call(
        line_kernel,
        in_specs=[whole(pltpu.SMEM), whole(), whole()],
        out_specs=whole(),
        out_shape=jax.ShapeDtypeStruct((copies, parts.shape[1], parts.shape[2]), BF16),
        compiler_params=pltpu.CompilerParams(vmem_limit_bytes=8 * 1024 * 1024),
    )(z, parts, targets)


def product_kernel(z_ref, parts_ref, part_ref, rows_ref, held):
    own = rows_ref.shape[0]
    total = parts_ref[0].astype(F32)
    for i in range(1, parts_ref.shape[0]):
        total = total + parts_ref[i].astype(F32)
    residual = total[:, :LANES]
    held[...] = residual
    part_ref[...] = lax.dot_general(
        total[:, LANES:], residual, (((0,), (0,)), ((), ())), precision=HIGHEST, preferred_element_type=F32
    )
    rows_ref[...] = held[pl.ds(pl.multiple_of(z_ref[0] * own, own), own), :]


def product(z, parts, own):
    return pl.pallas_call(
        product_kernel,
        in_specs=[whole(pltpu.SMEM), whole()],
        out_specs=[whole(), whole()],
        out_shape=[jax.ShapeDtypeStruct((LANES, LANES), F32), jax.ShapeDtypeStruct((own, LANES), F32)],
        scratch_shapes=[pltpu.VMEM((parts.shape[1], LANES), F32)],
        compiler_params=pltpu.CompilerParams(vmem_limit_bytes=8 * 1024 * 1024),
    )(z, parts)


Z_GROUPS = [[place(x, y, z, core) for z in range(NZ)] for x in range(NX) for y in range(NY) for core in range(2)]
PLANE_GROUPS = [[place(x, y, z, core) for x in range(NX) for y in range(NY)] for z in range(NZ) for core in range(2)]
FIRST_GROUPS = [[place(i, y, z, 0) for i in range(NX)] for y in range(NY) for z in range(NZ)] + [
    [place(x, i, z, 1) for i in range(NY)] for x in range(NX) for z in range(NZ)
]


def exchange(blocks, groups):
    return lax.all_to_all(blocks, BOTH, split_axis=0, concat_axis=0, tiled=True, axis_index_groups=groups)


def squares(rows):
    return jnp.sum(jnp.square(rows.astype(F32)), axis=1)[None, :]


def per_device(centres, coefficients, targets, batch_index, nys_index, eigvecs, eig_scale):
    own_centres, dim = centres.shape
    outputs = coefficients.shape[0]
    own_batch = targets.shape[1]
    own_nys = nys_index.shape[0]
    factor = -math.log2(math.e) / (0.7 * math.sqrt(dim))
    dev, grp = lax.axis_index("dev"), lax.axis_index("grp")
    z = (((dev >> 2) & 1) * 4 + (grp >> 1))[None]

    peer_centres = move(centres, CORE)
    own_copies, nys_rows = pick_rows(batch_index, nys_index, centres, NZ)
    own_copies, nys_rows, late_coefficients, late_centres = lax.optimization_barrier(
        (own_copies, nys_rows, coefficients, centres)
    )

    line = exchange(own_copies, Z_GROUPS)

    weights = jnp.pad(late_coefficients.astype(BF16), ((0, LANES - outputs), (0, 0)))
    centre_sq = squares(late_centres)
    weights, nys_rows = lax.optimization_barrier((weights, nys_rows))
    peer_weights = move(weights, CORE)
    peer_sq = move(centre_sq, CORE)
    nys_all = jnp.concatenate([nys_rows, move(nys_rows, CORE)], axis=0)
    nys_sq = squares(nys_all)
    basis = jnp.concatenate([eigvecs, move(eigvecs, CORE)], axis=0)
    line, weights, peer_weights, centre_sq, peer_sq, nys_all, nys_sq, basis = lax.optimization_barrier(
        (line, weights, peer_weights, centre_sq, peer_sq, nys_all, nys_sq, basis)
    )

    sheet = exchange(spread(NX, line.reshape(NZ * own_batch, dim)), FIRST_GROUPS).reshape(NX * NZ * own_batch, dim)
    shifts = (1, 2, 3)
    groups = [move(sheet, second_route(b)) for b in shifts]

    own_side = (centres, weights, centre_sq)
    own_start, peer_centres, peer_weights = score(factor, sheet, [own_side], fetch=(peer_centres, peer_weights))
    peer_side = (peer_centres, peer_weights, peer_sq)
    nothing = jnp.zeros_like(own_start)
    returned = []
    for b, rows in zip(shifts, groups):
        (part,) = score(factor, rows, [own_side, peer_side], rest=(nothing, nys_all, nys_sq, basis))
        returned.append(move(part, second_route(b)))
    sheet, own_start, *_ = lax.optimization_barrier((sheet, own_start, part))
    (part,) = score(factor, sheet, [peer_side], rest=(own_start, nys_all, nys_sq, basis))
    returned = [part, *returned]
    sheet_sum = functools.reduce(lambda s, r: s + r.astype(F32), returned[1:], returned[0].astype(F32))

    sheet_sum = sheet_sum.astype(BF16)
    parts = exchange(sheet_sum.reshape(NX, NZ * own_batch, 2 * LANES), FIRST_GROUPS)
    lines = exchange(line_sum(z, parts, targets, NZ), Z_GROUPS)
    part, residual_rows = product(z, lines, own_batch)
    residual_rows = residual_rows[:, :outputs]
    residual_own = residual_rows.T

    parts = exchange(spread(NX * NY, part, move(part, CORE)), PLANE_GROUPS)
    projected = jnp.sum(parts.astype(F32), axis=0)[:, :outputs]
    correction = jnp.dot(eigvecs, eig_scale[:, None] * projected, precision=HIGHEST)

    columns = lax.broadcasted_iota(jnp.int32, (own_batch + own_nys, own_centres), 1)
    chosen = (jnp.concatenate([batch_index, nys_index])[:, None] == columns).astype(F32)
    change = jnp.concatenate([-step_rate * residual_rows, step_rate * correction], axis=0)
    updated = coefficients + lax.dot_general(change, chosen, (((0,), (0,)), ((), ())), precision=HIGHEST)
    return (updated, residual_own)


def solution(mesh):
    in_specs = (
        P(BOTH, None),
        P(None, BOTH),
        P(None, BOTH),
        P(BOTH),
        P(BOTH),
        P(BOTH, None),
        P(),
    )
    out_specs = (P(None, BOTH), P(None, BOTH))
    return jax.shard_map(per_device, mesh=mesh, in_specs=in_specs, out_specs=out_specs, check_vma=False)
```
